32 devices in a mesh: face: 2 (over core), tile: 16 (over z, y, x).
Axes of the slice: x: 2, y: 2, z: 4, core: 2. Of those that a mesh axis runs over, the one named last changes fastest.
Arguments:
- crm_state: bfloat16 [6, 72, 32768], P(None, None, ('face', 'tile')), may hold values from -4 to 4
- active_levels: int32 [1024], P(('face', 'tile')), may hold values from 18 to 72
- mix_x: float32 [1024], P(('face', 'tile')), may hold values from 0.05 to 0.2
- drift_speed: float32 [1024], P(('face', 'tile')), may hold values from -0.1 to 0.1
- cond_rate: float32 [1024], P(('face', 'tile')), may hold values from 0.2 to 0.8
- mix_z: float32 [72], replicated, may hold values from 0.02 to 0.2
- point_mass: float32 [4096], P(('face', 'tile')), may hold values from 0.3 to 3
- neighbor_slots: int32 [4, 256], P(None, ('face', 'tile')), may hold values from 0 to 39, as said below
- edge_codes: int32 [4, 256], P(None, ('face', 'tile')), may hold values from 0 to 7, as said below
Outputs:
- new_state: bfloat16 [6, 72, 32768], P(None, None, ('face', 'tile'))
- gll_tendency: float32 [6, 72, 4096], P(None, None, ('face', 'tile'))
The draws below stay inside these ranges and needn't reach their ends.
Inputs may be any that keep to these rules, and one draw needn't show every extreme that they name: `neighbor_slots`: v // 8 is 0 for this device, 1 for tile index - 1, 2 for tile index + 1, 3 for face index - 1, 4 for face index + 1 (indices wrapping), and v % 8 the element there. The relation is mutual: if e names b across one of its edges, b names e across one of its own. On every device exactly 4 elements name an element on tile index - 1, 4 on tile index + 1, 2 on face index - 1 and 2 on face index + 1, each exactly one such element. `edge_codes`: 2 k' + r: k' is the neighbour's own edge that is shared, and r is 1 when the two elements list that edge's cells and points in opposite senses. Codes agree from both sides of every edge.
All inputs are finite; a program needn't handle non-finite values.
Results may differ from the reference program's by a relative error of at most 0.001.
Values sent between devices are 32-bit elements; how exact they have to be, the bound alone decides.
No kernel may reach another device: no remote copies, remote signals or barrier semaphores. Data moves between devices by JAX's collectives and lax.ppermute only.
A program may use at most 64 MiB of HBM per device.

```python
import math
import jax
import jax.numpy as jnp
import numpy as np
from jax import lax

FIELDS = 6
LEV = 72
CRMX = 32
NSUB = 2
BLK_R = 4
BLK_C = 2
E_DEV = 8
ELEMS = 256
N_FACE = 2
N_TILE = 16


def element_graph(key):
    graph_key = jax.random.fold_in(key, 11)
    turn_key, order_key = jax.random.split(graph_key)
    devices = N_FACE * N_TILE
    rotation = jax.random.randint(turn_key, (ELEMS,), 0, 4).astype(jnp.int32)

    def shuffle(device_key):
        return jax.random.permutation(device_key, E_DEV).astype(jnp.int32)
    layout = jax.vmap(shuffle)(jax.random.split(order_key, devices))
    inverse = jnp.argsort(layout, axis=1).astype(jnp.int32)
    element = jnp.arange(ELEMS, dtype=jnp.int32)
    device = element // E_DEV
    grid_place = layout[device, element % E_DEV]
    grid_rows = N_FACE * BLK_R
    grid_cols = N_TILE * BLK_C
    row_index = device // N_TILE * BLK_R + grid_place // BLK_C
    col_index = device % N_TILE * BLK_C + grid_place % BLK_C
    edge_ids = jnp.arange(4, dtype=jnp.int32)[:, None]
    facing = (edge_ids + rotation[None, :]) % 4
    row_step = jnp.array([-1, 0, 1, 0], jnp.int32)[facing]
    col_step = jnp.array([0, 1, 0, -1], jnp.int32)[facing]
    other_row = (row_index[None, :] + row_step) % grid_rows
    other_col = (col_index[None, :] + col_step) % grid_cols
    other_device = other_row // BLK_R * N_TILE + other_col // BLK_C
    other_place = other_row % BLK_R * BLK_C + other_col % BLK_C
    other_slot = inverse[other_device, other_place]
    other_element = other_device * E_DEV + other_slot
    source = jnp.where(other_device == device[None, :], 0, jnp.where(facing == 3, 1, jnp.where(facing == 1, 2, jnp.where(facing == 0, 3, 4))))
    slot_values = source * E_DEV + other_slot
    back_edge = (facing + 2 - rotation[other_element]) % 4
    sign_table = jnp.array([[1, 1, -1, -1], [1, -1, -1, 1]], jnp.int32)
    own_sign = sign_table[edge_ids % 2, rotation[None, :]]
    other_sign = sign_table[back_edge % 2, rotation[other_element]]
    code_values = 2 * back_edge + (own_sign != other_sign).astype(jnp.int32)
    return (slot_values.astype(jnp.int32), code_values.astype(jnp.int32))


def draw_neighbor_slots(key, part):
    return element_graph(key)[0]


def draw_edge_codes(key, part):
    return element_graph(key)[1]


def place_ends(entries, own_key, least, largest):
    longest = entries.shape.index(max(entries.shape))
    spots = []
    for shift in (0, 1):
        where = [jax.random.randint(jax.random.fold_in(own_key, axis), (), 0, length) for axis, length in enumerate(entries.shape)]
        where[longest] = (where[longest] + shift) % entries.shape[longest]
        spots.append(tuple(where))
    return entries.at[spots[0]].set(least).at[spots[1]].set(largest)


def block_scale(own_key, shape, cuts, low, high):
    gain, own = 1.0, jax.random.fold_in(own_key, 6)
    for dim, shards_of in cuts:
        draws = jnp.exp(jax.random.uniform(jax.random.fold_in(own, dim), (shards_of,), jnp.float32, low / len(cuts), high / len(cuts)))
        gain = gain * jnp.repeat(draws, shape[dim] // shards_of).reshape([-1 if axis == dim else 1 for axis in range(len(shape))])
    return gain


def normal_values(own_key, shape, deviation, most, shards=(), kind=jnp.bfloat16):
    entries = deviation * jax.random.normal(own_key, shape, jnp.float32)
    if shards:
        entries = entries * block_scale(own_key, shape, shards, -0.22, 0.18)
    return jnp.clip(entries, -most, most).astype(kind)


def setup_inputs(seed: int = 0) -> dict:
    key_list = jax.random.split(jax.random.key(seed), 10)
    crm_state = normal_values(key_list[0], (FIELDS, LEV, 4 * ELEMS * CRMX), 1.0, 4.0, ((2, 32),))
    active_levels = place_ends(jax.random.randint(key_list[1], (4 * ELEMS,), LEV // 4, LEV + 1), jax.random.fold_in(key_list[1], 1), LEV // 4, LEV).astype(jnp.int32)
    mix_x = jnp.clip(jnp.exp(math.log(0.2) - 1.3862944 * jax.random.uniform(key_list[2], (4 * ELEMS,), jnp.float32) ** block_scale(key_list[2], (4 * ELEMS,), ((0, 32),), -0.2, 0.2)), 0.05, 0.2)
    drift_speed = jnp.clip(jax.random.uniform(key_list[3], (4 * ELEMS,), jnp.float32, -0.1, 0.1) * block_scale(key_list[3], (4 * ELEMS,), ((0, 32),), -0.4, 0.0), -0.1, 0.1)
    cond_rate = jnp.clip(jnp.exp(math.log(0.8) - 1.3862944 * jax.random.uniform(key_list[4], (4 * ELEMS,), jnp.float32) ** block_scale(key_list[4], (4 * ELEMS,), ((0, 32),), -0.2, 0.2)), 0.2, 0.8)
    mix_z = jnp.clip(jnp.exp(jax.random.uniform(key_list[5], (LEV,), jnp.float32, math.log(0.02), math.log(0.2))), 0.02, 0.2)
    point_mass = jnp.clip(jnp.exp(math.log(3.0) - 2.3025851 * jax.random.uniform(key_list[6], (16 * ELEMS,), jnp.float32) ** block_scale(key_list[6], (16 * ELEMS,), ((0, 32),), -0.2, 0.2)), 0.3, 3.0)
    neighbor_slots = draw_neighbor_slots(jax.random.fold_in(key_list[9], 71), 0)
    edge_codes = draw_edge_codes(jax.random.fold_in(key_list[9], 71), 0)
    return dict(crm_state=crm_state, active_levels=active_levels, mix_x=mix_x, drift_speed=drift_speed, cond_rate=cond_rate, mix_z=mix_z, point_mass=point_mass, neighbor_slots=neighbor_slots, edge_codes=edge_codes)


per_time = 10.0
CELL_EDGE = [[0, 1], [1, 3], [2, 3], [0, 2]]
GLL_EDGE = [[0, 1, 2, 3], [3, 7, 11, 15], [12, 13, 14, 15], [0, 4, 8, 12]]

def oriented(edge_lists):
    row_list = []
    for edge_code in range(8):
        edge_side = list(edge_lists[edge_code // 2])
        if edge_code % 2 == 1:
            edge_side = edge_side[::-1]
        row_list.append(edge_side)
    return np.array(row_list, np.int32)

def lagrange(q, z):
    centres = [-1.5, -0.5, 0.5, 1.5]
    product = 1.0
    for r in range(4):
        if r != q:
            product = product * (z - centres[r]) / (centres[q] - centres[r])
    return product

def linear_weight(j, z):
    return 0.5 - z if j == 0 else 0.5 + z

def remap_matrix():
    gll_nodes = [-1.0, -1.0 / math.sqrt(5.0), 1.0 / math.sqrt(5.0), 1.0]
    matrix = [[0.0 for column in range(12)] for row in range(16)]
    for b in range(4):
        for a in range(4):
            p = 4 * b + a
            x = gll_nodes[a]
            y = gll_nodes[b]
            for j in range(2):
                for i in range(2):
                    matrix[p][2 * j + i] += 0.5 * linear_weight(j, y) * lagrange(1 + i, x) + 0.5 * linear_weight(i, x) * lagrange(1 + j, y)
            for m in range(2):
                matrix[p][4 + 6 + m] += 0.5 * linear_weight(m, y) * lagrange(0, x)
                matrix[p][4 + 2 + m] += 0.5 * linear_weight(m, y) * lagrange(3, x)
                matrix[p][4 + 0 + m] += 0.5 * linear_weight(m, x) * lagrange(0, y)
                matrix[p][4 + 4 + m] += 0.5 * linear_weight(m, x) * lagrange(3, y)
    return np.array(matrix, np.float32)

def microphysics(prognostic_bundle, alive_indicator, cond_speed):
    thermal_profile = prognostic_bundle[0]
    gaseous_moisture = prognostic_bundle[1]
    cloud_droplets = prognostic_bundle[2]
    icy_hydrometeor = prognostic_bundle[3]
    humidity_ceiling = 0.5 * jnp.exp(0.3 * thermal_profile)
    droplet_growth_increment = jnp.where(alive_indicator, jnp.maximum(cond_speed * (gaseous_moisture - humidity_ceiling), -cloud_droplets), 0.0)
    gaseous_moisture = gaseous_moisture - droplet_growth_increment
    cloud_droplets = cloud_droplets + droplet_growth_increment
    thermal_profile = thermal_profile + 0.5 * droplet_growth_increment
    glaciation_increment = jnp.where(alive_indicator, 0.3 * cloud_droplets * jax.nn.sigmoid(-2.0 * thermal_profile), 0.0)
    cloud_droplets = cloud_droplets - glaciation_increment
    icy_hydrometeor = icy_hydrometeor + glaciation_increment
    thermal_profile = thermal_profile + 0.1 * glaciation_increment
    return jnp.stack([thermal_profile, gaseous_moisture, cloud_droplets, icy_hydrometeor, prognostic_bundle[4], prognostic_bundle[5]])

def crm_advance(prognostic_bundle, active, mix_x, drift_speed, cond_rate, mix_z):
    initial = prognostic_bundle.astype(jnp.float32)
    levels = initial.shape[1]
    alive_indicator = jnp.arange(levels, dtype=jnp.int32)[:, None, None] < active[None, :, None]
    coupling = jnp.where(jnp.arange(levels, dtype=jnp.int32) < levels - 1, mix_z, 0.0)[:, None, None]
    mix_horiz = mix_x[:, None]
    shift_rate = drift_speed[:, None]
    cond_speed = cond_rate[:, None]
    current = initial
    for substep in range(NSUB):
        east_side = jnp.roll(current, -1, axis=3)
        west_side = jnp.roll(current, 1, axis=3)
        current = current + mix_horiz * (east_side - 2.0 * current + west_side) + 0.5 * shift_rate * (west_side - east_side)
        level_above = jnp.concatenate([current[:, 1:], current[:, -1:]], axis=1)
        flux_up = coupling * (level_above - current)
        flux_below = jnp.concatenate([jnp.zeros_like(flux_up[:, :1]), flux_up[:, :-1]], axis=1)
        current = current + flux_up - flux_below
        current = microphysics(current, alive_indicator, cond_speed)
    return (current, lax.optimization_barrier(jnp.mean(current - initial, axis=3)) * per_time)

def reference(crm_state, active_levels, mix_x, drift_speed, cond_rate, mix_z, point_mass, neighbor_slots, edge_codes):
    columns = 4 * E_DEV
    blocks = ELEMS // E_DEV

    def advance_block(block_index):
        begin = block_index * columns
        piece = lax.dynamic_slice_in_dim(crm_state, begin * CRMX, columns * CRMX, 2).reshape(FIELDS, LEV, columns, CRMX)
        current, tendency = crm_advance(piece, lax.dynamic_slice_in_dim(active_levels, begin, columns, 0), lax.dynamic_slice_in_dim(mix_x, begin, columns, 0), lax.dynamic_slice_in_dim(drift_speed, begin, columns, 0), lax.dynamic_slice_in_dim(cond_rate, begin, columns, 0), mix_z)
        return (current.astype(jnp.bfloat16).reshape(FIELDS, LEV, columns * CRMX), tendency)
    states, tendencies = lax.map(advance_block, jnp.arange(blocks, dtype=jnp.int32))
    new_state = jnp.transpose(states, (1, 2, 0, 3)).reshape(FIELDS, LEV, 4 * ELEMS * CRMX)
    tendency = jnp.transpose(tendencies, (1, 2, 0, 3)).reshape(FIELDS, LEV, 4 * ELEMS)
    element = jnp.arange(ELEMS, dtype=jnp.int32)
    device = element // E_DEV
    face_index = device // N_TILE
    tile_index = device % N_TILE
    source = neighbor_slots // E_DEV
    position = neighbor_slots % E_DEV
    face_other = jnp.where(source == 3, (face_index - 1) % N_FACE, jnp.where(source == 4, (face_index + 1) % N_FACE, face_index))
    tile_other = jnp.where(source == 1, (tile_index - 1) % N_TILE, jnp.where(source == 2, (tile_index + 1) % N_TILE, tile_index))
    partner = ((face_other * N_TILE + tile_other) * E_DEV + position).astype(jnp.int32)
    cell_table = jnp.asarray(oriented(CELL_EDGE))
    cell_pick = jnp.take(cell_table, edge_codes, axis=0)
    gather_index = (partner[:, :, None] * 4 + cell_pick).transpose(1, 0, 2).reshape(-1).astype(jnp.int32)
    across = jnp.take(tendency, gather_index, axis=2).reshape(FIELDS, LEV, ELEMS, 8)
    stacked = jnp.concatenate([tendency.reshape(FIELDS, LEV, ELEMS, 4), across], axis=3)
    matrix = jnp.asarray(remap_matrix(), jnp.float32)
    gll = jnp.einsum('flec,pc->flep', stacked, matrix, precision=lax.Precision.HIGHEST)
    masses = point_mass.reshape(ELEMS, 16)
    weighted = gll * masses
    numerator = weighted
    denominator = masses
    flat_weighted = weighted.reshape(FIELDS, LEV, ELEMS * 16)
    flat_mass = point_mass
    point_table = jnp.asarray(oriented(GLL_EDGE))
    for k in range(4):
        point_index = (partner[k][:, None] * 16 + jnp.take(point_table, edge_codes[k], axis=0)).reshape(-1).astype(jnp.int32)
        numerator = numerator.at[:, :, :, GLL_EDGE[k]].add(jnp.take(flat_weighted, point_index, axis=2).reshape(FIELDS, LEV, ELEMS, 4))
        denominator = denominator.at[:, GLL_EDGE[k]].add(jnp.take(flat_mass, point_index).reshape(ELEMS, 4))
    gll_tendency = (numerator / denominator).reshape(FIELDS, LEV, 16 * ELEMS)
    return (new_state, gll_tendency)
```

```python
import functools
import math

import jax
import jax.numpy as jnp
import numpy as np
from jax import lax
from jax.experimental import pallas as pl
from jax.experimental.pallas import tpu as pltpu
from jax.sharding import PartitionSpec as P

NSUB = 2
BLK_R = 4
BLK_C = 2
PER_TIME = 10.0
LANES = 128
HI = lax.Precision.HIGHEST
F32 = jnp.float32
BF16 = jnp.bfloat16
I32 = jnp.int32

CELL_EDGE = [[0, 1], [1, 3], [2, 3], [0, 2]]
GLL_EDGE = [[0, 1, 2, 3], [3, 7, 11, 15], [12, 13, 14, 15], [0, 4, 8, 12]]


def lagrange(q, z):
    centres = [-1.5, -0.5, 0.5, 1.5]
    product = 1.0
    for r in range(4):
        if r != q:
            product = product * (z - centres[r]) / (centres[q] - centres[r])
    return product


def linear_weight(j, z):
    return 0.5 - z if j == 0 else 0.5 + z


GLL_NODES = [-1.0, -1.0 / math.sqrt(5.0), 1.0 / math.sqrt(5.0), 1.0]


def remap_matrix():
    matrix = [[0.0 for column in range(12)] for row in range(16)]
    for b in range(4):
        for a in range(4):
            p = 4 * b + a
            x = GLL_NODES[a]
            y = GLL_NODES[b]
            for j in range(2):
                for i in range(2):
                    matrix[p][2 * j + i] += 0.5 * linear_weight(j, y) * lagrange(
                        1 + i, x
                    ) + 0.5 * linear_weight(i, x) * lagrange(1 + j, y)
            for m in range(2):
                matrix[p][4 + 6 + m] += 0.5 * linear_weight(m, y) * lagrange(0, x)
                matrix[p][4 + 2 + m] += 0.5 * linear_weight(m, y) * lagrange(3, x)
                matrix[p][4 + 0 + m] += 0.5 * linear_weight(m, x) * lagrange(0, y)
                matrix[p][4 + 4 + m] += 0.5 * linear_weight(m, x) * lagrange(3, y)
    return np.array(matrix, np.float32)


class Sizes:
    def __init__(self, elements, flat_len):
        self.elements = elements
        self.edges = 4 * elements
        self.cells = 4 * elements
        self.points = 16 * elements
        self.raw = 2 * BLK_R
        self.part = 4 * BLK_R
        self.flat = flat_len
        self.wide = -(-(flat_len + 2) // LANES) * LANES
        self.columns = 2 * self.cells + 4 * self.raw
        self.ops = self.columns + 8
        self.face_rows = self.cells + 2 * self.raw + 8
        self.tile_rows = 2 * self.raw + self.part


def constant_tables(size):
    matrix = remap_matrix()
    across_t = np.zeros((2 * size.edges, size.points), np.float32)
    own_t = np.zeros((size.cells, size.points), np.float32)
    spread_t = np.zeros((4 * size.edges, size.points), np.float32)
    for e in range(size.elements):
        for p in range(16):
            for c in range(4):
                own_t[4 * e + c, 16 * e + p] = matrix[p][c]
            for k in range(4):
                for m in range(2):
                    row = m * size.edges + k * size.elements + e
                    across_t[row, 16 * e + p] = matrix[p][4 + 2 * k + m]
        for k in range(4):
            for t in range(4):
                row = t * size.edges + k * size.elements + e
                spread_t[row, 16 * e + GLL_EDGE[k][t]] = 1.0
    return np.concatenate([across_t, own_t, spread_t], axis=0)


def edge_weight(t, m):
    return 0.5 * linear_weight(m, GLL_NODES[t]) * lagrange(0, -1.0)


def iota(shape, dim):
    return lax.broadcasted_iota(I32, shape, dim)


def dot_nn(a, b, precision=HI):
    return lax.dot_general(
        a, b, (((1,), (0,)), ((), ())), precision=precision, preferred_element_type=F32
    )


def dot_nt(a, b, precision=HI):
    return lax.dot_general(
        a, b, (((1,), (1,)), ((), ())), precision=precision, preferred_element_type=F32
    )


def dot_tn(a, b, precision=HI):
    return lax.dot_general(
        a, b, (((0,), (0,)), ((), ())), precision=precision, preferred_element_type=F32
    )


def flat_row(table):
    return jnp.concatenate([table[k : k + 1, :] for k in range(4)], axis=1)


def twice(row):
    return jnp.concatenate([row, row], axis=1)


def side_slots(size, side, order):
    n = size.edges
    key = jnp.where(side >= 0, side * 2 * n + order, 8 * n)
    eye = iota((n, n), 0) == iota((n, n), 1)
    wide = jnp.broadcast_to(key.astype(F32), (n, n))
    column = jnp.sum(jnp.where(eye, wide, 0.0), axis=1, keepdims=True)
    floor = jnp.broadcast_to((side * 2 * n).astype(F32), (n, n))
    lower = jnp.logical_and(column < wide, column >= floor)
    count = jnp.sum(jnp.where(lower, 1.0, 0.0), axis=0, keepdims=True).astype(I32)
    return jnp.where(side >= 0, count, 0)


def edge_cell(k, m):
    odd = k & 1
    base = jnp.where(k == 2, 2, odd * jnp.where(k == 1, 1, 0))
    return base + m * (1 + odd)


def edge_point(k, t):
    odd = k & 1
    base = jnp.where(k == 2, 12, jnp.where(k == 1, 3, 0))
    return base + t * (1 + 3 * odd)


class Edges:
    def __init__(self, size, slots_row, codes_row, parity):
        n = size.edges
        flat = iota((1, n), 1)
        self.k = flat // size.elements
        self.e = flat % size.elements
        self.source = slots_row // size.elements
        self.place = slots_row % size.elements
        self.other_k = codes_row // 2
        self.turned = codes_row % 2
        self.side = jnp.where(
            self.source == 2 - parity, 0, jnp.where(self.source == 1 + parity, 1, -1)
        )
        self.flat = flat
        self.other_flat = self.other_k * size.elements + self.place


def gather_matrix_t(size, edges, slot, twin):
    cells, raw = size.cells, size.raw
    rows = []
    for m in range(2):
        mm = jnp.where(edges.turned == 1, 1 - m, m)
        cell = 4 * edges.place + edge_cell(edges.other_k, mm)
        local = jnp.where(edges.source == 0, cells * twin, cells * (1 - twin)) + cell
        far = 2 * cells + 2 * raw * edges.side + raw * twin + 2 * slot + mm
        rows.append(jnp.where(edges.side >= 0, far, local))
    target = jnp.concatenate(rows, axis=1)
    return jnp.where(iota((size.columns, 2 * size.edges), 0) == target, 1.0, 0.0)


def operator_t(size, tables, gather_t, mass_row, twin):
    across_t = tables[0 : 2 * size.edges, :]
    own_t = tables[2 * size.edges : 2 * size.edges + size.cells, :]
    from_across = dot_nn(gather_t, across_t)
    zero = jnp.zeros((size.cells, size.points), F32)
    placed = [zero, own_t] if twin else [own_t, zero]
    rest = jnp.zeros((size.columns - 2 * size.cells, size.points), F32)
    full = from_across + jnp.concatenate(placed + [rest], axis=0)
    tail = jnp.where(iota((8, size.points), 0) == 0, 1.0, 0.0)
    return jnp.concatenate([full, tail], axis=0) * mass_row


def spread_of(size, tables):
    start = 2 * size.edges + size.cells
    return tables[start : start + 4 * size.edges, :]


def crm_kernel(
    size,
    levels,
    width,
    state_ref,
    active_ref,
    mix_ref,
    drift_ref,
    cond_ref,
    mixz_ref,
    slots_ref,
    codes_ref,
    mass_ref,
    new_ref,
    face_ref,
    in_buf,
    out_buf,
    in_sem,
    out_sem,
):
    fields = in_buf.shape[1]
    per_lane = LANES // width

    def load(e):
        return pltpu.make_async_copy(
            state_ref.at[:, :, pl.ds(e * LANES, LANES)], in_buf.at[e], in_sem.at[e]
        )

    def save(e):
        return pltpu.make_async_copy(
            out_buf.at[e], new_ref.at[:, :, pl.ds(e * LANES, LANES)], out_sem.at[e]
        )

    for e in range(size.elements):
        load(e).start()

    eye = iota((levels, levels), 0) == iota((levels, levels), 1)
    mixz = jnp.broadcast_to(mixz_ref[...], (levels, levels))
    couple = jnp.sum(jnp.where(eye, mixz, 0.0), axis=1, keepdims=True)
    couple = jnp.where(iota((levels, 1), 0) < levels - 1, couple, 0.0)
    couple = jnp.broadcast_to(couple, (levels, LANES))
    level = iota((levels, LANES), 0)
    lane = iota((1, LANES), 1)
    group = lane // width
    at_last = jnp.broadcast_to(lane % width == width - 1, (levels, LANES))
    at_first = jnp.broadcast_to(lane % width == 0, (levels, LANES))

    def lanes_of(ref, e):
        row = jnp.full((1, LANES), ref[e * per_lane], ref.dtype)
        for c in range(1, per_lane):
            row = jnp.where(group == c, ref[e * per_lane + c], row)
        return row

    def element(e):
        load(e).wait()
        mix = lanes_of(mix_ref, e)
        half = 0.5 * lanes_of(drift_ref, e)
        rate = jnp.broadcast_to(lanes_of(cond_ref, e), (levels, LANES))
        alive = level < lanes_of(active_ref, e)
        centre = jnp.broadcast_to(1.0 - 2.0 * mix, (levels, LANES))
        east_c = jnp.broadcast_to(mix - half, (levels, LANES))
        west_c = jnp.broadcast_to(mix + half, (levels, LANES))

        def transport(a):
            east = jnp.where(
                at_last, pltpu.roll(a, width - 1, 1), pltpu.roll(a, LANES - 1, 1)
            )
            west = jnp.where(
                at_first, pltpu.roll(a, LANES - width + 1, 1), pltpu.roll(a, 1, 1)
            )
            a = centre * a + east_c * east + west_c * west
            flux = couple * (pltpu.roll(a, levels - 1, 0) - a)
            return a + flux - pltpu.roll(flux, 1, 0)

        start = [in_buf[e, f].astype(F32) for f in range(fields)]
        cur = list(start)
        for substep in range(NSUB):
            cur = [transport(a) for a in cur]
            t, qv, ql, qi = cur[:4]
            sat = 0.5 * jnp.exp(0.3 * t)
            cond = jnp.where(alive, jnp.maximum(rate * (qv - sat), -ql), 0.0)
            qv = qv - cond
            ql = ql + cond
            t = t + 0.5 * cond
            freeze = jnp.where(alive, 0.15 * ql * (1.0 - jnp.tanh(t)), 0.0)
            ql = ql - freeze
            qi = qi + freeze
            t = t + 0.1 * freeze
            cur[:4] = [t, qv, ql, qi]
        for f in range(fields):
            out_buf[e, f] = cur[f].astype(BF16)
        save(e).start()
        return jnp.concatenate([cur[f] - start[f] for f in range(fields)], axis=0)

    pair_lanes = 2 * LANES
    cell_of = iota((2 * per_lane, pair_lanes), 1) // width
    mean = jnp.where(iota((2 * per_lane, pair_lanes), 0) == cell_of, PER_TIME / width, 0.0)
    mean = mean.astype(BF16)
    face_ref[...] = jnp.zeros(face_ref.shape, F32)

    def pair(i, carry):
        diff = jnp.concatenate([element(2 * i), element(2 * i + 1)], axis=1)
        high = diff.astype(BF16)
        low = (diff - high.astype(F32)).astype(BF16)
        rows = dot_nt(mean, high, None) + dot_nt(mean, low, None)
        face_ref[pl.ds(pl.multiple_of(i * 2 * per_lane, 8), 2 * per_lane), 0 : size.flat] = rows
        return carry

    lax.fori_loop(0, size.elements // 2, pair, 0)

    parity = lax.axis_index("tile") % 2
    slots_row = flat_row(slots_ref[...])
    codes_row = flat_row(codes_ref[...])
    edges = Edges(size, slots_row, codes_row, parity)
    slot = side_slots(size, edges.side, edges.flat)
    rows = 2 * size.raw
    place = jnp.where(edges.side >= 0, edges.side * size.raw + 2 * slot, -8)
    put = jnp.concatenate([place, place + 1], axis=1)
    select = jnp.where(iota((rows, 2 * size.edges), 0) == put, 1.0, 0.0)
    cell = jnp.concatenate(
        [4 * edges.e + edge_cell(edges.k, m) for m in range(2)], axis=1
    )
    cell_t = jnp.where(iota((size.cells, 2 * size.edges), 0) == cell, 1.0, 0.0)
    pick = dot_nt(select, cell_t, None)
    face_ref[size.cells : size.cells + rows, :] = dot_nn(pick, face_ref[0 : size.cells, :])
    base = size.cells + rows
    face_ref[base : base + 1, 0 : size.edges] = slots_row.astype(F32)
    face_ref[base + 1 : base + 2, 0 : size.edges] = codes_row.astype(F32)
    face_ref[base + 2 : base + 3, 0 : size.points] = mass_ref[...]

    for e in range(size.elements):
        save(e).wait()


def weights_kernel(size, slots_ref, codes_ref, mass_ref, table_ref, part_ref):
    parity = lax.axis_index("tile") % 2
    edges = Edges(size, flat_row(slots_ref[...]), flat_row(codes_ref[...]), parity)
    tables = table_ref[...]
    slot_far = side_slots(size, edges.side, edges.other_flat)
    oper_t = operator_t(
        size, tables, gather_matrix_t(size, edges, slot_far, 0), mass_ref[...], False
    )
    slot = side_slots(size, edges.side, edges.flat)
    rows = 2 * size.part
    first = jnp.where(edges.side >= 0, edges.side * size.part + 4 * slot, -8)
    put = jnp.concatenate([first + t for t in range(4)], axis=1)
    select = jnp.where(iota((rows, 4 * size.edges), 0) == put, 1.0, 0.0)
    points = dot_nn(select, spread_of(size, tables), None)
    part = dot_nt(points, oper_t)
    n = size.elements
    both = jnp.zeros((1, n), I32)
    hits = []
    for s in range(2):
        hit = jnp.where(edges.side == s, 1, 0)
        total = hit[:, 0:n]
        for k in range(1, 4):
            total = total + hit[:, k * n : (k + 1) * n]
        hits.append(total)
    both = jnp.where(jnp.logical_and(hits[0] > 0, hits[1] > 0), 1.0, 0.0)
    flag = jnp.max(both)
    part_ref[:, 0 : size.ops] = part
    part_ref[:, size.ops :] = jnp.full((rows, LANES - size.ops), flag, F32)


def message_kernel(size, own_ref, twin_ref, part_ref, even_ref, odd_ref):
    cells = jnp.concatenate([own_ref[0 : size.cells, :], twin_ref[0 : size.cells, :]], axis=0)
    part = dot_nn(part_ref[:, 0 : 2 * size.cells], cells)
    lane = iota((2 * size.part, size.wide), 1)
    part = jnp.where(lane == size.flat, part_ref[:, size.columns : size.columns + 1], part)
    part = jnp.where(lane == size.flat + 1, part_ref[:, size.ops : size.ops + 1], part)
    for s, ref in enumerate((even_ref, odd_ref)):
        first = size.cells + s * size.raw
        ref[0 : size.raw, :] = own_ref[first : first + size.raw, :]
        ref[size.raw : 2 * size.raw, :] = twin_ref[first : first + size.raw, :]
        ref[2 * size.raw :, :] = part[s * size.part : (s + 1) * size.part, :]


def inner_kernel(
    size,
    slots_ref,
    codes_ref,
    mass_ref,
    table_ref,
    own_ref,
    twin_ref,
    sum_ref,
    near_ref,
    matrix_ref,
):
    parity = lax.axis_index("tile") % 2
    tables = table_ref[...]
    base = size.cells + 2 * size.raw
    own = Edges(size, flat_row(slots_ref[...]), flat_row(codes_ref[...]), parity)
    twin = Edges(
        size,
        twin_ref[base : base + 1, 0 : size.edges].astype(I32),
        twin_ref[base + 1 : base + 2, 0 : size.edges].astype(I32),
        parity,
    )
    twin_mass = twin_ref[base + 2 : base + 3, 0 : size.points]
    own_slot = side_slots(size, own.side, own.other_flat)
    twin_slot = side_slots(size, twin.side, twin.other_flat)
    oper = jnp.concatenate(
        [
            operator_t(size, tables, gather_matrix_t(size, own, own_slot, 0), mass_ref[...], False),
            operator_t(size, tables, gather_matrix_t(size, twin, twin_slot, 1), twin_mass, True),
        ],
        axis=1,
    )
    far = 2 * size.points
    targets = []
    for t in range(4):
        tt = jnp.where(own.turned == 1, 3 - t, t)
        point = 16 * own.place + edge_point(own.other_k, tt)
        local = jnp.where(own.source == 0, 0, size.points) + point
        targets.append(
            jnp.where(own.side >= 0, far + own.side * size.part + 4 * own_slot + tt, local)
        )
    target = jnp.concatenate(targets, axis=1)
    rows = far + 2 * size.part
    partner_t = jnp.where(iota((rows, 4 * size.edges), 0) == target, 1.0, 0.0)
    assemble_t = dot_nn(partner_t, spread_of(size, tables), None)
    eye = jnp.where(iota((far, size.points), 0) == iota((far, size.points), 1), 1.0, 0.0)
    total_t = dot_nn(oper, assemble_t[0:far, :] + eye)
    cells = 2 * size.cells
    matrix_ref[0 : 4 * size.raw, :] = total_t[cells : size.columns, :]
    matrix_ref[4 * size.raw : 4 * size.raw + 2 * size.part, :] = assemble_t[far:, :]
    matrix_ref[4 * size.raw + 2 * size.part :, :] = total_t[size.columns :, :]
    chip = jnp.concatenate([own_ref[0 : size.cells, :], twin_ref[0 : size.cells, :]], axis=0)
    sum_ref[...] = dot_tn(chip[:, 0 : size.flat], total_t[0:cells, :])
    side_slot = jnp.where(own.side >= 0, own.side * BLK_R + own_slot, -1)
    match = jnp.broadcast_to(twice(side_slot), (2 * size.part, 2 * size.edges)) == (
        iota((2 * size.part, 2 * size.edges), 0) // 4
    )
    t_of = iota((2 * size.part, 2 * size.edges), 0) % 4
    m_of = iota((2 * size.part, 2 * size.edges), 1) // size.edges
    weight = jnp.zeros(match.shape, F32)
    for t in range(4):
        for m in range(2):
            here = jnp.logical_and(t_of == t, m_of == m)
            weight = jnp.where(here, edge_weight(t, m), weight)
    weight = jnp.where(match, weight, 0.0)
    cell = jnp.concatenate(
        [
            4 * own.e + edge_cell(own.k, jnp.where(own.turned == 1, 1 - m, m))
            for m in range(2)
        ],
        axis=1,
    )
    cell_t = jnp.where(iota((size.cells, 2 * size.edges), 0) == cell, 1.0, 0.0)
    near_ref[...] = dot_nn(dot_nt(weight, cell_t), own_ref[0 : size.cells, :])


def final_kernel(size, even_ref, odd_ref, sum_ref, near_ref, matrix_ref, out_ref, keep_ref):
    raw = 2 * size.raw
    mass = jnp.concatenate(
        [ref[raw:, size.flat : size.flat + 1] for ref in (even_ref, odd_ref)], axis=0
    )
    part = jnp.concatenate([even_ref[raw:, :], odd_ref[raw:, :]], axis=0)
    part = part + mass * near_ref[...]
    rows = jnp.concatenate([even_ref[0:raw, :], odd_ref[0:raw, :], part], axis=0)
    n = 2 * raw + 2 * size.part
    side = matrix_ref[2 * raw : n, :]
    total = sum_ref[...] + dot_tn(rows[:, 0 : size.flat], matrix_ref[0:n, :])
    mass_sum = matrix_ref[n : n + 1, :] + jnp.sum(side * mass, axis=0, keepdims=True)
    out_ref[...] = total / mass_sum
    keep_ref[0:1, :] = mass_sum
    row = jnp.concatenate(
        [ref[raw : raw + 1, size.flat + 1 : size.flat + 2] for ref in (even_ref, odd_ref)], axis=0
    )
    keep_ref[1:3, :] = jnp.broadcast_to(row, (2, size.points))
    keep_ref[3:, :] = jnp.zeros((5, size.points), F32)


VMEM = pl.BlockSpec(memory_space=pltpu.VMEM)
SMEM = pl.BlockSpec(memory_space=pltpu.SMEM)
ANY = pl.BlockSpec(memory_space=pl.ANY)


def call(body, name, outs, ins, in_specs=None, out_specs=None, scratch=(), limit=8):
    return pl.pallas_call(
        body,
        out_shape=outs,
        in_specs=in_specs or [VMEM] * len(ins),
        out_specs=out_specs or [VMEM] * len(outs),
        scratch_shapes=scratch,
        compiler_params=pltpu.CompilerParams(vmem_limit_bytes=limit * 1024 * 1024),
        name=name,
    )(*ins)


def shape_of(*dims):
    return jax.ShapeDtypeStruct(dims, F32)


def advance(size, crm_state, column_args, mix_z, slots, codes, mass_row):
    fields, levels, lanes = crm_state.shape
    width = lanes // column_args[0].shape[0]
    buffers = (size.elements, fields, levels, LANES)
    return call(
        functools.partial(crm_kernel, size, levels, width),
        "advance",
        [jax.ShapeDtypeStruct(crm_state.shape, BF16), shape_of(size.face_rows, size.wide)],
        [crm_state, *column_args, mix_z.reshape(1, levels), slots, codes, mass_row],
        in_specs=[ANY] + [SMEM] * 4 + [VMEM] * 4,
        out_specs=[ANY, VMEM],
        scratch=[
            pltpu.VMEM(buffers, BF16),
            pltpu.VMEM(buffers, BF16),
            pltpu.SemaphoreType.DMA((size.elements,)),
            pltpu.SemaphoreType.DMA((size.elements,)),
        ],
        limit=16,
    )


def swap_pairs(odd):
    tiles = lax.axis_size("tile")
    pairs = []
    for t in range(tiles):
        up = (t % 2 == 0) != odd
        pairs.append((t, (t + 1 if up else t - 1) % tiles))
    return pairs


def swap(value, odd):
    return lax.ppermute(value, "tile", swap_pairs(odd))


def shift(value, axis, steps):
    count = lax.axis_size(axis)
    return lax.ppermute(value, axis, [(s, (s + steps) % count) for s in range(count)])


def assemble_pair(size, face, slots, codes, mass_row):
    tables = jnp.asarray(constant_tables(size))
    twin = shift(face, "face", 1)
    (part,) = call(
        functools.partial(weights_kernel, size),
        "weights",
        [shape_of(2 * size.part, LANES)],
        [slots, codes, mass_row, tables],
    )
    message = shape_of(size.tile_rows, size.wide)
    even, odd = call(
        functools.partial(message_kernel, size), "message", [message] * 2, [face, twin, part]
    )
    odd_in = swap(odd, True)
    even_in = swap(even, False)
    extra = 4 * size.raw + 2 * size.part
    inner, near, matrix = call(
        functools.partial(inner_kernel, size),
        "inner",
        [
            shape_of(size.flat, size.points),
            shape_of(2 * size.part, size.wide),
            shape_of(extra + 8, size.points),
        ],
        [slots, codes, mass_row, tables, face, twin],
    )
    out, keep = call(
        functools.partial(final_kernel, size),
        "final",
        [shape_of(size.flat, size.points), shape_of(8, size.points)],
        [even_in, odd_in, inner, near, matrix],
    )
    return out, part, keep, matrix, even_in, odd_in


def second_exchange(size, out, part, keep, matrix, even_in, odd_in):
    raw = 2 * size.raw
    mine = part[0, size.ops] > 0.0
    inputs = (even_in, odd_in)
    for s in range(2):
        source = inputs[1 - s]
        first = 2 * size.cells + raw * (1 - s)
        weights = part[s * size.part : (s + 1) * size.part, first : first + raw]
        side = matrix[2 * raw + s * size.part : 2 * raw + (s + 1) * size.part, :]
        wanted = jnp.logical_or(mine, keep[1 + s, 0] > 0.0)

        def add(value, s=s, source=source, weights=weights, side=side):
            sent = jnp.dot(weights, source[0:raw, 0 : size.flat], precision=HI)
            got = swap(sent, s == 1)
            return value + jnp.dot(got.T, side, precision=HI) / keep[0:1, :]

        out = lax.cond(wanted, add, lambda value: value, out)
    return out


def local(
    crm_state,
    active_levels,
    mix_x,
    drift_speed,
    cond_rate,
    mix_z,
    point_mass,
    neighbor_slots,
    edge_codes,
):
    fields, levels, _ = crm_state.shape
    size = Sizes(neighbor_slots.shape[1], fields * levels)
    mass_row = point_mass.reshape(1, size.points)
    new_state, face = advance(
        size,
        crm_state,
        (active_levels, mix_x, drift_speed, cond_rate),
        mix_z,
        neighbor_slots,
        edge_codes,
        mass_row,
    )
    results = assemble_pair(size, face, neighbor_slots, edge_codes, mass_row)
    out = second_exchange(size, *results)
    return (new_state, out.reshape(fields, levels, size.points))


def solution(mesh):
    in_specs = (
        P(None, None, ("face", "tile")),
        P(("face", "tile")),
        P(("face", "tile")),
        P(("face", "tile")),
        P(("face", "tile")),
        P(),
        P(("face", "tile")),
        P(None, ("face", "tile")),
        P(None, ("face", "tile")),
    )
    out_specs = (P(None, None, ("face", "tile")), P(None, None, ("face", "tile")))
    return jax.shard_map(local, mesh=mesh, in_specs=in_specs, out_specs=out_specs, check_vma=False)
```

```python
import functools
import math

import jax
import jax.numpy as jnp
import numpy as np
from jax import lax
from jax.experimental import pallas as pl
from jax.experimental.pallas import tpu as pltpu
from jax.sharding import PartitionSpec as P

NSUB = 2
BLK_R = 4
BLK_C = 2
PER_TIME = 10.0
LANES = 128
HI = lax.Precision.HIGHEST
F32 = jnp.float32
BF16 = jnp.bfloat16
I32 = jnp.int32

CELL_EDGE = [[0, 1], [1, 3], [2, 3], [0, 2]]
GLL_EDGE = [[0, 1, 2, 3], [3, 7, 11, 15], [12, 13, 14, 15], [0, 4, 8, 12]]


def lagrange(q, z):
    centres = [-1.5, -0.5, 0.5, 1.5]
    product = 1.0
    for r in range(4):
        if r != q:
            product = product * (z - centres[r]) / (centres[q] - centres[r])
    return product


def linear_weight(j, z):
    return 0.5 - z if j == 0 else 0.5 + z


GLL_NODES = [-1.0, -1.0 / math.sqrt(5.0), 1.0 / math.sqrt(5.0), 1.0]


def remap_matrix():
    matrix = [[0.0 for column in range(12)] for row in range(16)]
    for b in range(4):
        for a in range(4):
            p = 4 * b + a
            x = GLL_NODES[a]
            y = GLL_NODES[b]
            for j in range(2):
                for i in range(2):
                    matrix[p][2 * j + i] += 0.5 * linear_weight(j, y) * lagrange(
                        1 + i, x
                    ) + 0.5 * linear_weight(i, x) * lagrange(1 + j, y)
            for m in range(2):
                matrix[p][4 + 6 + m] += 0.5 * linear_weight(m, y) * lagrange(0, x)
                matrix[p][4 + 2 + m] += 0.5 * linear_weight(m, y) * lagrange(3, x)
                matrix[p][4 + 0 + m] += 0.5 * linear_weight(m, x) * lagrange(0, y)
                matrix[p][4 + 4 + m] += 0.5 * linear_weight(m, x) * lagrange(3, y)
    return np.array(matrix, np.float32)


class Sizes:
    def __init__(self, elements, flat_len):
        self.elements = elements
        self.edges = 4 * elements
        self.cells = 4 * elements
        self.points = 16 * elements
        self.raw = 2 * BLK_R
        self.part = 4 * BLK_R
        self.flat = flat_len
        self.wide = -(-(flat_len + 2) // LANES) * LANES
        self.columns = 2 * self.cells + 4 * self.raw
        self.ops = self.columns + 8
        self.face_rows = self.cells + 2 * self.raw + 8
        self.tile_rows = 2 * self.raw + self.part


def constant_tables(size):
    matrix = remap_matrix()
    across_t = np.zeros((2 * size.edges, size.points), np.float32)
    own_t = np.zeros((size.cells, size.points), np.float32)
    spread_t = np.zeros((4 * size.edges, size.points), np.float32)
    for e in range(size.elements):
        for p in range(16):
            for c in range(4):
                own_t[4 * e + c, 16 * e + p] = matrix[p][c]
            for k in range(4):
                for m in range(2):
                    row = m * size.edges + k * size.elements + e
                    across_t[row, 16 * e + p] = matrix[p][4 + 2 * k + m]
        for k in range(4):
            for t in range(4):
                row = t * size.edges + k * size.elements + e
                spread_t[row, 16 * e + GLL_EDGE[k][t]] = 1.0
    return np.concatenate([across_t, own_t, spread_t], axis=0)


def edge_weight(t, m):
    return 0.5 * linear_weight(m, GLL_NODES[t]) * lagrange(0, -1.0)


def iota(shape, dim):
    return lax.broadcasted_iota(I32, shape, dim)


def dot_nn(a, b, precision=HI):
    return lax.dot_general(
        a, b, (((1,), (0,)), ((), ())), precision=precision, preferred_element_type=F32
    )


def dot_nt(a, b, precision=HI):
    return lax.dot_general(
        a, b, (((1,), (1,)), ((), ())), precision=precision, preferred_element_type=F32
    )


def dot_tn(a, b, precision=HI):
    return lax.dot_general(
        a, b, (((0,), (0,)), ((), ())), precision=precision, preferred_element_type=F32
    )


def flat_row(table):
    return jnp.concatenate([table[k : k + 1, :] for k in range(4)], axis=1)


def twice(row):
    return jnp.concatenate([row, row], axis=1)


def side_slots(size, side, order):
    n = size.edges
    key = jnp.where(side >= 0, side * 2 * n + order, 8 * n)
    eye = iota((n, n), 0) == iota((n, n), 1)
    wide = jnp.broadcast_to(key.astype(F32), (n, n))
    column = jnp.sum(jnp.where(eye, wide, 0.0), axis=1, keepdims=True)
    floor = jnp.broadcast_to((side * 2 * n).astype(F32), (n, n))
    lower = jnp.logical_and(column < wide, column >= floor)
    count = jnp.sum(jnp.where(lower, 1.0, 0.0), axis=0, keepdims=True).astype(I32)
    return jnp.where(side >= 0, count, 0)


def edge_cell(k, m):
    odd = k & 1
    base = jnp.where(k == 2, 2, odd * jnp.where(k == 1, 1, 0))
    return base + m * (1 + odd)


def edge_point(k, t):
    odd = k & 1
    base = jnp.where(k == 2, 12, jnp.where(k == 1, 3, 0))
    return base + t * (1 + 3 * odd)


class Edges:
    def __init__(self, size, slots_row, codes_row, parity):
        n = size.edges
        flat = iota((1, n), 1)
        self.k = flat // size.elements
        self.e = flat % size.elements
        self.source = slots_row // size.elements
        self.place = slots_row % size.elements
        self.other_k = codes_row // 2
        self.turned = codes_row % 2
        self.side = jnp.where(
            self.source == 2 - parity, 0, jnp.where(self.source == 1 + parity, 1, -1)
        )
        self.flat = flat
        self.other_flat = self.other_k * size.elements + self.place


def gather_matrix_t(size, edges, slot, twin):
    cells, raw = size.cells, size.raw
    rows = []
    for m in range(2):
        mm = jnp.where(edges.turned == 1, 1 - m, m)
        cell = 4 * edges.place + edge_cell(edges.other_k, mm)
        local = jnp.where(edges.source == 0, cells * twin, cells * (1 - twin)) + cell
        far = 2 * cells + 2 * raw * edges.side + raw * twin + 2 * slot + mm
        rows.append(jnp.where(edges.side >= 0, far, local))
    target = jnp.concatenate(rows, axis=1)
    return jnp.where(iota((size.columns, 2 * size.edges), 0) == target, 1.0, 0.0)


def operator_t(size, tables, gather_t, mass_row, twin):
    across_t = tables[0 : 2 * size.edges, :]
    own_t = tables[2 * size.edges : 2 * size.edges + size.cells, :]
    from_across = dot_nn(gather_t, across_t)
    zero = jnp.zeros((size.cells, size.points), F32)
    placed = [zero, own_t] if twin else [own_t, zero]
    rest = jnp.zeros((size.columns - 2 * size.cells, size.points), F32)
    full = from_across + jnp.concatenate(placed + [rest], axis=0)
    tail = jnp.where(iota((8, size.points), 0) == 0, 1.0, 0.0)
    return jnp.concatenate([full, tail], axis=0) * mass_row


def spread_of(size, tables):
    start = 2 * size.edges + size.cells
    return tables[start : start + 4 * size.edges, :]


SUBLANES = 8


def crm_kernel(size, levels, width, count, *refs):
    state_hbm, given = refs[0], refs[1 : 1 + count]
    new_ref, face_ref = refs[1 + count : 3 + count]
    held = refs[3 + count : 3 + 2 * count]
    state_ref, table_ref, wide_ref, out_buf, base_ref, inc_ref, state_sem, held_sem = refs[
        3 + 2 * count :
    ]
    fields = state_ref.shape[0]
    steps = levels // SUBLANES
    per_lane = LANES // width
    full = (SUBLANES, LANES)
    lane = iota(full, 1)
    pair_lanes = 2 * LANES
    pairs = size.elements // 2

    def load(p):
        lanes = pl.ds(pl.multiple_of(p * pair_lanes, pair_lanes), pair_lanes)
        return pltpu.make_async_copy(
            state_hbm.at[:, :, lanes], state_ref.at[:, :, lanes], state_sem.at[p]
        )

    small = [
        pltpu.make_async_copy(src, dst, held_sem.at[n])
        for n, (src, dst) in enumerate(zip(given, held))
    ]
    for copy in small:
        copy.start()
    for p in range(pairs):
        load(p).start()
    table_ref[...] = jnp.zeros(table_ref.shape, F32)
    base_ref[...] = jnp.zeros(base_ref.shape, F32)
    inc_ref[...] = jnp.zeros(inc_ref.shape, F32)
    for copy in small:
        copy.wait()
    first = 0
    for ref in held:
        rows, lanes = ref.shape
        table_ref[first : first + rows, 0:lanes] = ref[...].astype(F32)
        first += rows
    params = table_ref[...]

    def spread(ref, i):
        return ref[pl.ds(i, SUBLANES, stride=steps), :]

    eye = iota((levels, LANES), 0) == iota((levels, LANES), 1)
    mixz = jnp.broadcast_to(params[4:5, :], (levels, LANES))
    couple = jnp.sum(jnp.where(eye, mixz, 0.0), axis=1, keepdims=True)
    couple = jnp.where(iota((levels, 1), 0) < levels - 1, couple, 0.0)
    wide_ref[0, 0] = jnp.broadcast_to(couple, (levels, LANES))
    coupling = [spread(wide_ref.at[0, 0], i) for i in range(steps)]

    def vertical(a):
        above = a[1:] + [pltpu.roll(a[0], SUBLANES - 1, 0)]
        flux = [c * (u - v) for c, u, v in zip(coupling, above, a)]
        below = [pltpu.roll(flux[-1], 1, 0)] + flux[:-1]
        return [v + f - b for v, f, b in zip(a, flux, below)]

    level = [iota(full, 0) * steps + i for i in range(steps)]
    first = lane - lane % width
    east_lane = first + (lane + 1) % width
    west_lane = first + (lane + width - 1) % width

    def lanes_of(value, index):
        return jnp.take_along_axis(value, index, axis=1)

    def element(e, half):
        here = lanes_of(params[0:SUBLANES, :], e * per_lane + lane // width)

        def row(r):
            return jnp.broadcast_to(here[r : r + 1, :], full)

        active, mix, drift, rate = row(0).astype(I32), row(1), row(2), row(3)
        centre, east_c, west_c = 1.0 - 2.0 * mix, mix - 0.5 * drift, mix + 0.5 * drift
        alive = [v < active for v in level]
        ice = [jnp.where(v, 0.15, 0.0) for v in alive]
        lanes = pl.ds(pl.multiple_of(e * LANES, LANES), LANES)

        def transport(a):
            a = [
                centre * v + east_c * lanes_of(v, east_lane) + west_c * lanes_of(v, west_lane)
                for v in a
            ]
            return vertical(a)

        cur = []
        for f in range(fields):
            wide_ref[half, f] = state_ref[f, :, lanes].astype(F32)
            cur.append([spread(wide_ref.at[half, f], i) for i in range(steps)])
        changes = []
        for substep in range(NSUB):
            cur = [transport(a) for a in cur]
            conds, freezes = [], []
            for i in range(steps):
                t, qv, ql, qi = [cur[f][i] for f in range(4)]
                sat = jnp.exp2((0.3 * math.log2(math.e)) * t - 1.0)
                cond = jnp.where(alive[i], jnp.maximum(rate * (qv - sat), -ql), 0.0)
                ql = ql + cond
                t = t + 0.5 * cond
                freeze = ice[i] * ql * (1.0 - jnp.tanh(t))
                cur[0][i] = t + 0.1 * freeze
                cur[1][i] = qv - cond
                cur[2][i] = ql - freeze
                cur[3][i] = qi + freeze
                conds.append(cond)
                freezes.append(freeze)
            changes += conds + freezes
        for f in range(fields):
            for i in range(steps):
                out_buf[half, f, pl.ds(i, SUBLANES, stride=steps), :] = cur[f][i]
            new_ref[f, :, lanes] = out_buf[half, f].astype(BF16)
        return jnp.concatenate(changes, axis=0)

    cells = pair_lanes // width
    group = iota((pair_lanes, LANES), 0) // width == iota((pair_lanes, LANES), 1) % cells
    total = jnp.where(group, 1.0, 0.0).astype(BF16)

    def pair(p, carry):
        load(p).wait()
        mine = lane // cells == p
        lanes = pl.ds(pl.multiple_of(p * pair_lanes, pair_lanes), pair_lanes)
        for f in range(fields):
            sums = dot_nn(state_ref[f, :, lanes], total, None)
            keep = jnp.broadcast_to(mine[0:1, :], sums.shape)
            base_ref[f] = jnp.where(keep, sums, base_ref[f])
        change = jnp.concatenate([element(2 * p, 0), element(2 * p + 1, 1)], axis=1)
        high = change.astype(BF16)
        low = (change - high.astype(F32)).astype(BF16)
        sums = dot_nn(high, total, None) + dot_nn(low, total, None)
        keep = jnp.broadcast_to(mine[0:1, :], sums.shape)
        inc_ref[...] = jnp.where(keep, sums, inc_ref[...])
        return carry

    lax.fori_loop(0, pairs, pair, 0)

    def change_of(n):
        return [
            inc_ref[(n * steps + i) * SUBLANES : (n * steps + i + 1) * SUBLANES, :]
            for i in range(steps)
        ]

    parts = [[change_of(2 * n), change_of(2 * n + 1)] for n in range(NSUB)]
    parity = lax.axis_index("tile") % 2
    slots_row = flat_row(params[6:10, 0 : size.elements])
    codes_row = flat_row(params[10:14, 0 : size.elements])
    edges = Edges(size, slots_row.astype(I32), codes_row.astype(I32), parity)
    slot = side_slots(size, edges.side, edges.flat)
    rows = 2 * size.raw
    place = jnp.where(edges.side >= 0, size.cells + edges.side * size.raw + 2 * slot, -8)
    put = jnp.concatenate([place, place + 1], axis=1)
    cell = jnp.concatenate(
        [4 * edges.e + edge_cell(edges.k, m) for m in range(2)], axis=1
    )
    select = jnp.where(iota((LANES, 2 * size.edges), 0) == put, 1.0, 0.0)
    cell = jnp.broadcast_to(cell.astype(F32), (SUBLANES, 2 * size.edges))
    picked = dot_nt(cell, select, None).astype(I32)
    source = jnp.where(lane < size.cells, lane, picked)

    scale = PER_TIME / width
    columns = []
    for f in range(fields):
        start = [spread(base_ref.at[f], i) for i in range(steps)]
        mean = start
        for cond, freeze in parts:
            mean = vertical(mean)
            if f == 0:
                mean = [v + 0.5 * c + 0.1 * z for v, c, z in zip(mean, cond, freeze)]
            elif f == 1:
                mean = [v - c for v, c in zip(mean, cond)]
            elif f == 2:
                mean = [v + c - z for v, c, z in zip(mean, cond, freeze)]
            elif f == 3:
                mean = [v + z for v, z in zip(mean, freeze)]
        columns += [lanes_of(scale * (v - s), source) for v, s in zip(mean, start)]
    columns.append(jnp.zeros((size.wide - size.flat, LANES), F32))
    tendency = jnp.concatenate(columns, axis=0)
    base = size.cells + rows
    face_ref[0:base, :] = tendency.T[0:base, :]
    face_ref[base:, :] = jnp.zeros((SUBLANES, size.wide), F32)
    face_ref[base : base + 1, 0 : size.edges] = slots_row
    face_ref[base + 1 : base + 2, 0 : size.edges] = codes_row
    face_ref[base + 2 : base + 3, 0 : size.points] = params[5:6, 0 : size.points]


def face_edges(size, face_ref, parity):
    base = size.cells + 2 * size.raw
    slots_row = face_ref[base : base + 1, 0 : size.edges].astype(I32)
    codes_row = face_ref[base + 1 : base + 2, 0 : size.edges].astype(I32)
    mass_row = face_ref[base + 2 : base + 3, 0 : size.points]
    return Edges(size, slots_row, codes_row, parity), mass_row


def weights_kernel(size, own_ref, table_ref, part_ref):
    parity = lax.axis_index("tile") % 2
    edges, mass_row = face_edges(size, own_ref, parity)
    tables = table_ref[...]
    slot_far = side_slots(size, edges.side, edges.other_flat)
    oper_t = operator_t(
        size, tables, gather_matrix_t(size, edges, slot_far, 0), mass_row, False
    )
    slot = side_slots(size, edges.side, edges.flat)
    rows = 2 * size.part
    first = jnp.where(edges.side >= 0, edges.side * size.part + 4 * slot, -8)
    put = jnp.concatenate([first + t for t in range(4)], axis=1)
    select = jnp.where(iota((rows, 4 * size.edges), 0) == put, 1.0, 0.0)
    points = dot_nn(select, spread_of(size, tables), None)
    part = dot_nt(points, oper_t)
    n = size.elements
    both = jnp.zeros((1, n), I32)
    hits = []
    for s in range(2):
        hit = jnp.where(edges.side == s, 1, 0)
        total = hit[:, 0:n]
        for k in range(1, 4):
            total = total + hit[:, k * n : (k + 1) * n]
        hits.append(total)
    both = jnp.where(jnp.logical_and(hits[0] > 0, hits[1] > 0), 1.0, 0.0)
    flag = jnp.max(both)
    part_ref[:, 0 : size.ops] = part
    part_ref[:, size.ops :] = jnp.full((rows, LANES - size.ops), flag, F32)


def message_kernel(size, own_ref, twin_ref, part_ref, even_ref, odd_ref):
    cells = jnp.concatenate([own_ref[0 : size.cells, :], twin_ref[0 : size.cells, :]], axis=0)
    part = dot_nn(part_ref[:, 0 : 2 * size.cells], cells)
    lane = iota((2 * size.part, size.wide), 1)
    part = jnp.where(lane == size.flat, part_ref[:, size.columns : size.columns + 1], part)
    part = jnp.where(lane == size.flat + 1, part_ref[:, size.ops : size.ops + 1], part)
    for s, ref in enumerate((even_ref, odd_ref)):
        first = size.cells + s * size.raw
        ref[0 : size.raw, :] = own_ref[first : first + size.raw, :]
        ref[size.raw : 2 * size.raw, :] = twin_ref[first : first + size.raw, :]
        ref[2 * size.raw :, :] = part[s * size.part : (s + 1) * size.part, :]


def inner_kernel(
    size, table_ref, own_ref, twin_ref, state_ref, sum_ref, near_ref, matrix_ref, new_ref, sem
):
    save = pltpu.make_async_copy(state_ref, new_ref, sem)
    save.start()
    parity = lax.axis_index("tile") % 2
    tables = table_ref[...]
    own, own_mass = face_edges(size, own_ref, parity)
    twin, twin_mass = face_edges(size, twin_ref, parity)
    own_slot = side_slots(size, own.side, own.other_flat)
    twin_slot = side_slots(size, twin.side, twin.other_flat)
    oper = jnp.concatenate(
        [
            operator_t(size, tables, gather_matrix_t(size, own, own_slot, 0), own_mass, False),
            operator_t(size, tables, gather_matrix_t(size, twin, twin_slot, 1), twin_mass, True),
        ],
        axis=1,
    )
    far = 2 * size.points
    targets = []
    for t in range(4):
        tt = jnp.where(own.turned == 1, 3 - t, t)
        point = 16 * own.place + edge_point(own.other_k, tt)
        local = jnp.where(own.source == 0, 0, size.points) + point
        targets.append(
            jnp.where(own.side >= 0, far + own.side * size.part + 4 * own_slot + tt, local)
        )
    target = jnp.concatenate(targets, axis=1)
    rows = far + 2 * size.part
    partner_t = jnp.where(iota((rows, 4 * size.edges), 0) == target, 1.0, 0.0)
    assemble_t = dot_nn(partner_t, spread_of(size, tables), None)
    eye = jnp.where(iota((far, size.points), 0) == iota((far, size.points), 1), 1.0, 0.0)
    total_t = dot_nn(oper, assemble_t[0:far, :] + eye)
    cells = 2 * size.cells
    matrix_ref[0 : 4 * size.raw, :] = total_t[cells : size.columns, :]
    matrix_ref[4 * size.raw : 4 * size.raw + 2 * size.part, :] = assemble_t[far:, :]
    matrix_ref[4 * size.raw + 2 * size.part :, :] = total_t[size.columns :, :]
    chip = jnp.concatenate([own_ref[0 : size.cells, :], twin_ref[0 : size.cells, :]], axis=0)
    sum_ref[...] = dot_tn(chip[:, 0 : size.flat], total_t[0:cells, :])
    side_slot = jnp.where(own.side >= 0, own.side * BLK_R + own_slot, -1)
    match = jnp.broadcast_to(twice(side_slot), (2 * size.part, 2 * size.edges)) == (
        iota((2 * size.part, 2 * size.edges), 0) // 4
    )
    t_of = iota((2 * size.part, 2 * size.edges), 0) % 4
    m_of = iota((2 * size.part, 2 * size.edges), 1) // size.edges
    weight = jnp.zeros(match.shape, F32)
    for t in range(4):
        for m in range(2):
            here = jnp.logical_and(t_of == t, m_of == m)
            weight = jnp.where(here, edge_weight(t, m), weight)
    weight = jnp.where(match, weight, 0.0)
    cell = jnp.concatenate(
        [
            4 * own.e + edge_cell(own.k, jnp.where(own.turned == 1, 1 - m, m))
            for m in range(2)
        ],
        axis=1,
    )
    cell_t = jnp.where(iota((size.cells, 2 * size.edges), 0) == cell, 1.0, 0.0)
    near_ref[...] = dot_nn(dot_nt(weight, cell_t), own_ref[0 : size.cells, :])
    save.wait()


def final_kernel(
    size,
    levels,
    even_ref,
    odd_ref,
    sum_ref,
    near_ref,
    matrix_ref,
    part_ref,
    out_ref,
    keep_ref,
    flag_ref,
):
    raw = 2 * size.raw
    mine = part_ref[0:1, size.ops : size.ops + 1]
    others = [ref[raw : raw + 1, size.flat + 1 : size.flat + 2] for ref in (even_ref, odd_ref)]
    flag = jnp.where(mine + others[0] + others[1] > 0.0, 1.0, 0.0)
    flag_ref[0, 0] = jnp.sum(flag).astype(I32)
    mass = jnp.concatenate(
        [ref[raw:, size.flat : size.flat + 1] for ref in (even_ref, odd_ref)], axis=0
    )
    part = jnp.concatenate([even_ref[raw:, :], odd_ref[raw:, :]], axis=0)
    part = part + mass * near_ref[...]
    rows = jnp.concatenate([even_ref[0:raw, :], odd_ref[0:raw, :], part], axis=0)
    n = 2 * raw + 2 * size.part
    side = matrix_ref[2 * raw : n, :]
    mass_sum = matrix_ref[n : n + 1, :] + jnp.sum(side * mass, axis=0, keepdims=True)
    keep_ref[...] = jnp.broadcast_to(mass_sum, (8, size.points))
    total = sum_ref[...] + dot_tn(rows[:, 0 : size.flat], matrix_ref[0:n, :])
    total = total / mass_sum
    steps = levels // SUBLANES
    for f in range(size.flat // levels):
        for i in range(steps):
            row = (f * steps + i) * SUBLANES
            out_ref[pl.ds(f * levels + i, SUBLANES, stride=steps), :] = total[row : row + SUBLANES, :]


VMEM = pl.BlockSpec(memory_space=pltpu.VMEM)
SMEM = pl.BlockSpec(memory_space=pltpu.SMEM)
HBM = pl.BlockSpec(memory_space=pltpu.HBM)


def call(body, name, outs, ins, in_specs=None, out_specs=None, scratch=(), limit=8):
    return pl.pallas_call(
        body,
        out_shape=outs,
        in_specs=in_specs or [VMEM] * len(ins),
        out_specs=out_specs or [VMEM] * len(outs),
        scratch_shapes=scratch,
        compiler_params=pltpu.CompilerParams(vmem_limit_bytes=limit * 1024 * 1024),
        name=name,
    )(*ins)


def shape_of(*dims):
    return jax.ShapeDtypeStruct(dims, F32)


def advance(size, crm_state, params):
    fields, levels, lanes = crm_state.shape
    width = lanes // size.cells
    block = pltpu.VMEM((2, fields, levels, LANES), F32)
    params = [value.reshape(-1, value.shape[-1]) for value in params]
    rows = sum(value.shape[0] for value in params)
    ins = [pltpu.with_memory_space_constraint(value, pltpu.HBM) for value in (crm_state, *params)]
    return call(
        functools.partial(crm_kernel, size, levels, width, len(params)),
        "advance",
        [
            pltpu.VMEM(crm_state.shape, BF16),
            pltpu.VMEM((size.face_rows, size.wide), F32),
        ],
        ins,
        in_specs=[HBM] * len(ins),
        scratch=[pltpu.VMEM(value.shape, value.dtype) for value in params]
        + [
            pltpu.VMEM(crm_state.shape, BF16),
            pltpu.VMEM((-(-rows // SUBLANES) * SUBLANES, LANES), F32),
            block,
            block,
            pltpu.VMEM((fields, levels, LANES), F32),
            pltpu.VMEM((2 * NSUB * levels, LANES), F32),
            pltpu.SemaphoreType.DMA((size.elements // 2,)),
            pltpu.SemaphoreType.DMA((len(params),)),
        ],
        limit=16,
    )


def swap_pairs(odd):
    tiles = lax.axis_size("tile")
    pairs = []
    for t in range(tiles):
        up = (t % 2 == 0) != odd
        pairs.append((t, (t + 1 if up else t - 1) % tiles))
    return pairs


def swap(value, odd):
    return lax.ppermute(value, "tile", swap_pairs(odd))


def shift(value, axis, steps):
    count = lax.axis_size(axis)
    return lax.ppermute(value, axis, [(s, (s + steps) % count) for s in range(count)])


def assemble_pair(size, levels, state, face):
    tables = jnp.asarray(constant_tables(size))
    twin = shift(face, "face", 1)
    (part,) = call(
        functools.partial(weights_kernel, size),
        "weights",
        [shape_of(2 * size.part, LANES)],
        [face, tables],
    )
    message = shape_of(size.tile_rows, size.wide)
    even, odd = call(
        functools.partial(message_kernel, size), "message", [message] * 2, [face, twin, part]
    )
    odd_in = swap(odd, True)
    even_in = swap(even, False)
    extra = 4 * size.raw + 2 * size.part
    inner, near, matrix, new_state = call(
        functools.partial(inner_kernel, size),
        "inner",
        [
            shape_of(size.flat, size.points),
            shape_of(2 * size.part, size.wide),
            shape_of(extra + 8, size.points),
            pltpu.HBM(state.shape, state.dtype),
        ],
        [tables, face, twin, pltpu.with_memory_space_constraint(state, pltpu.VMEM)],
        out_specs=[VMEM, VMEM, VMEM, HBM],
        scratch=[pltpu.SemaphoreType.DMA],
    )
    out, keep, flag = call(
        functools.partial(final_kernel, size, levels),
        "final",
        [
            pltpu.VMEM((size.flat, size.points), F32),
            shape_of(8, size.points),
            pltpu.SMEM((1, 1), I32),
        ],
        [even_in, odd_in, inner, near, matrix, part],
        out_specs=[VMEM, VMEM, SMEM],
    )
    return new_state, (out, part, keep, matrix, even_in, odd_in, flag)


def one_of(index, branches, *operands):
    whole = jax.make_jaxpr(lambda i, *rest: lax.switch(i, branches, *rest))(index, *operands)
    last = whole.jaxpr.eqns[-1]
    return last.primitive.bind(index, *operands, **last.params)[0]


def second_exchange(size, levels, out, part, keep, matrix, even_in, odd_in, flag):
    raw = 2 * size.raw

    def add(s, value, part, keep, matrix, even_in, odd_in):
        source = (odd_in, even_in)[s]
        first = 2 * size.cells + raw * (1 - s)
        weights = part[s * size.part : (s + 1) * size.part, first : first + raw]
        side = matrix[2 * raw + s * size.part : 2 * raw + (s + 1) * size.part, :]
        sent = jnp.dot(weights, source[0:raw, 0 : size.flat], precision=HI)
        got = swap(sent, s == 1)
        more = jnp.dot(got.T, side, precision=HI) / keep[0:1, :]
        more = more.reshape(-1, levels // SUBLANES, SUBLANES, size.points)
        return value + more.transpose(0, 2, 1, 3).reshape(value.shape)

    def none(value, *rest):
        return value

    def some(value, *rest):
        mine = rest[0][0, size.ops]
        for s, received in ((0, rest[3]), (1, rest[4])):
            other = received[raw, size.flat + 1]
            value = lax.cond(
                mine + other > 0.0, functools.partial(add, s), none, value, *rest
            )
        return value

    operands = (out, part, keep, matrix, even_in, odd_in)
    return one_of(flag[0, 0], (none, some), *operands)


def oriented(edge_lists):
    rows = []
    for code in range(8):
        side = list(edge_lists[code // 2])
        rows.append(side[::-1] if code % 2 == 1 else side)
    return np.array(rows, np.int32)


def collect(value, slots):
    pieces = [value]
    for axis, steps in (("tile", 1), ("tile", -1), ("face", 1), ("face", -1)):
        pieces.append(shift(value, axis, steps))
    return jnp.concatenate(pieces, axis=0), slots


def assemble_any(size, levels, face, masses, slots, codes):
    elements = size.elements
    cells = face[0 : size.cells, 0 : size.flat].reshape(elements, 4, size.flat)
    pool, rows = collect(cells, slots)
    pick = jnp.take(jnp.asarray(oriented(CELL_EDGE)), codes, axis=0)
    index = (rows[:, :, None] * 4 + pick).transpose(1, 0, 2).reshape(-1)
    across = jnp.take(pool.reshape(-1, size.flat), index, axis=0)
    stacked = jnp.concatenate([cells, across.reshape(elements, 8, size.flat)], axis=1)
    points = jnp.einsum("ecz,pc->epz", stacked, jnp.asarray(remap_matrix()), precision=HI)
    masses = masses.reshape(elements, 16)
    numerator, denominator = points * masses[:, :, None], masses
    weighted, rows = collect(numerator, slots)
    mass_pool, _ = collect(masses, slots)
    pick = jnp.take(jnp.asarray(oriented(GLL_EDGE)), codes, axis=0)
    for k in range(4):
        index = (rows[k][:, None] * 16 + pick[k]).reshape(-1)
        got = jnp.take(weighted.reshape(-1, size.flat), index, axis=0)
        numerator = numerator.at[:, GLL_EDGE[k]].add(got.reshape(elements, 4, size.flat))
        got = jnp.take(mass_pool.reshape(-1), index)
        denominator = denominator.at[:, GLL_EDGE[k]].add(got.reshape(elements, 4))
    ratio = (numerator / denominator[:, :, None]).reshape(size.points, size.flat)
    ratio = ratio.reshape(size.points, -1, levels // SUBLANES, SUBLANES)
    return ratio.transpose(1, 3, 2, 0).reshape(size.flat, size.points)


def local(
    crm_state,
    active_levels,
    mix_x,
    drift_speed,
    cond_rate,
    mix_z,
    point_mass,
    neighbor_slots,
    edge_codes,
):
    fields, levels, _ = crm_state.shape
    size = Sizes(neighbor_slots.shape[1], fields * levels)
    params = (
        active_levels,
        mix_x,
        drift_speed,
        cond_rate,
        mix_z,
        point_mass,
        neighbor_slots,
        edge_codes,
    )
    state, face = advance(size, crm_state, params)
    tiles = lax.axis_size("tile")
    if lax.axis_size("face") == 2 and tiles % 2 == 0 and tiles > 2:
        new_state, results = assemble_pair(size, levels, state, face)
        out = second_exchange(size, levels, *results)
    else:
        new_state = state
        out = assemble_any(size, levels, face, point_mass, neighbor_slots, edge_codes)
    return (new_state, out.reshape(fields, levels, size.points))


def solution(mesh):
    in_specs = (
        P(None, None, ("face", "tile")),
        P(("face", "tile")),
        P(("face", "tile")),
        P(("face", "tile")),
        P(("face", "tile")),
        P(),
        P(("face", "tile")),
        P(None, ("face", "tile")),
        P(None, ("face", "tile")),
    )
    out_specs = (P(None, None, ("face", "tile")), P(None, None, ("face", "tile")))
    return jax.shard_map(local, mesh=mesh, in_specs=in_specs, out_specs=out_specs, check_vma=False)
```

```python
import functools
import math

import jax
import jax.numpy as jnp
import numpy as np
from jax import lax
from jax.experimental import pallas as pl
from jax.experimental.pallas import tpu as pltpu
from jax.sharding import PartitionSpec as P

NSUB = 2
BLK_R = 4
BLK_C = 2
PER_TIME = 10.0
LANES = 128
HI = lax.Precision.HIGHEST
F32 = jnp.float32
BF16 = jnp.bfloat16
I32 = jnp.int32

CELL_EDGE = [[0, 1], [1, 3], [2, 3], [0, 2]]
GLL_EDGE = [[0, 1, 2, 3], [3, 7, 11, 15], [12, 13, 14, 15], [0, 4, 8, 12]]


def lagrange(q, z):
    centres = [-1.5, -0.5, 0.5, 1.5]
    product = 1.0
    for r in range(4):
        if r != q:
            product = product * (z - centres[r]) / (centres[q] - centres[r])
    return product


def linear_weight(j, z):
    return 0.5 - z if j == 0 else 0.5 + z


GLL_NODES = [-1.0, -1.0 / math.sqrt(5.0), 1.0 / math.sqrt(5.0), 1.0]


def remap_matrix():
    matrix = [[0.0 for column in range(12)] for row in range(16)]
    for b in range(4):
        for a in range(4):
            p = 4 * b + a
            x = GLL_NODES[a]
            y = GLL_NODES[b]
            for j in range(2):
                for i in range(2):
                    matrix[p][2 * j + i] += 0.5 * linear_weight(j, y) * lagrange(
                        1 + i, x
                    ) + 0.5 * linear_weight(i, x) * lagrange(1 + j, y)
            for m in range(2):
                matrix[p][4 + 6 + m] += 0.5 * linear_weight(m, y) * lagrange(0, x)
                matrix[p][4 + 2 + m] += 0.5 * linear_weight(m, y) * lagrange(3, x)
                matrix[p][4 + 0 + m] += 0.5 * linear_weight(m, x) * lagrange(0, y)
                matrix[p][4 + 4 + m] += 0.5 * linear_weight(m, x) * lagrange(3, y)
    return np.array(matrix, np.float32)


class Sizes:
    def __init__(self, elements, flat_len):
        self.elements = elements
        self.edges = 4 * elements
        self.cells = 4 * elements
        self.points = 16 * elements
        self.raw = 2 * BLK_R
        self.part = 4 * BLK_R
        self.flat = flat_len
        self.wide = -(-(flat_len + 2) // LANES) * LANES
        self.columns = 2 * self.cells + 4 * self.raw
        self.ops = self.columns + 8
        self.face_rows = self.cells + 2 * self.raw + 8
        self.tile_rows = 2 * self.raw + self.part


def constant_tables(size):
    matrix = remap_matrix()
    across_t = np.zeros((2 * size.edges, size.points), np.float32)
    own_t = np.zeros((size.cells, size.points), np.float32)
    spread_t = np.zeros((4 * size.edges, size.points), np.float32)
    for e in range(size.elements):
        for p in range(16):
            for c in range(4):
                own_t[4 * e + c, 16 * e + p] = matrix[p][c]
            for k in range(4):
                for m in range(2):
                    row = m * size.edges + k * size.elements + e
                    across_t[row, 16 * e + p] = matrix[p][4 + 2 * k + m]
        for k in range(4):
            for t in range(4):
                row = t * size.edges + k * size.elements + e
                spread_t[row, 16 * e + GLL_EDGE[k][t]] = 1.0
    return np.concatenate([across_t, own_t, spread_t], axis=0)


def edge_weight(t, m):
    return 0.5 * linear_weight(m, GLL_NODES[t]) * lagrange(0, -1.0)


def iota(shape, dim):
    return lax.broadcasted_iota(I32, shape, dim)


def dot_nn(a, b, precision=HI):
    return lax.dot_general(
        a, b, (((1,), (0,)), ((), ())), precision=precision, preferred_element_type=F32
    )


def dot_nt(a, b, precision=HI):
    return lax.dot_general(
        a, b, (((1,), (1,)), ((), ())), precision=precision, preferred_element_type=F32
    )


def dot_tn(a, b, precision=HI):
    return lax.dot_general(
        a, b, (((0,), (0,)), ((), ())), precision=precision, preferred_element_type=F32
    )


def split(value):
    high = value.astype(BF16)
    return high, (value - high.astype(F32)).astype(BF16)


def stack_left(value, axis):
    high, low = split(value)
    return jnp.concatenate([high, low, high], axis=axis)


def stack_right(value, axis):
    high, low = split(value)
    return jnp.concatenate([high, high, low], axis=axis)


def flat_row(table):
    return jnp.concatenate([table[k : k + 1, :] for k in range(4)], axis=1)


def twice(row):
    return jnp.concatenate([row, row], axis=1)


def side_slots(size, side, order):
    n = size.edges
    key = jnp.where(side >= 0, side * 2 * n + order, 8 * n)
    eye = iota((n, n), 0) == iota((n, n), 1)
    wide = jnp.broadcast_to(key.astype(F32), (n, n))
    column = jnp.sum(jnp.where(eye, wide, 0.0), axis=1, keepdims=True)
    floor = jnp.broadcast_to((side * 2 * n).astype(F32), (n, n))
    lower = jnp.logical_and(column < wide, column >= floor)
    count = jnp.sum(jnp.where(lower, 1.0, 0.0), axis=0, keepdims=True).astype(I32)
    return jnp.where(side >= 0, count, 0)


def edge_cell(k, m):
    odd = k & 1
    base = jnp.where(k == 2, 2, odd * jnp.where(k == 1, 1, 0))
    return base + m * (1 + odd)


def edge_point(k, t):
    odd = k & 1
    base = jnp.where(k == 2, 12, jnp.where(k == 1, 3, 0))
    return base + t * (1 + 3 * odd)


class Edges:
    def __init__(self, size, slots_row, codes_row, parity):
        n = size.edges
        flat = iota((1, n), 1)
        self.k = flat // size.elements
        self.e = flat % size.elements
        self.source = slots_row // size.elements
        self.place = slots_row % size.elements
        self.other_k = codes_row // 2
        self.turned = codes_row % 2
        self.side = jnp.where(
            self.source == 2 - parity, 0, jnp.where(self.source == 1 + parity, 1, -1)
        )
        self.flat = flat
        self.other_flat = self.other_k * size.elements + self.place


def gather_matrix_t(size, edges, slot, twin):
    cells, raw = size.cells, size.raw
    rows = []
    for m in range(2):
        mm = jnp.where(edges.turned == 1, 1 - m, m)
        cell = 4 * edges.place + edge_cell(edges.other_k, mm)
        local = jnp.where(edges.source == 0, cells * twin, cells * (1 - twin)) + cell
        far = 2 * cells + 2 * raw * edges.side + raw * twin + 2 * slot + mm
        rows.append(jnp.where(edges.side >= 0, far, local))
    target = jnp.concatenate(rows, axis=1)
    return jnp.where(iota((size.columns, 2 * size.edges), 0) == target, 1.0, 0.0)


def operator_t(size, tables, gather_t, mass_row, twin):
    across_t = tables[0 : 2 * size.edges, :]
    own_t = tables[2 * size.edges : 2 * size.edges + size.cells, :]
    from_across = dot_nn(gather_t, across_t)
    zero = jnp.zeros((size.cells, size.points), F32)
    placed = [zero, own_t] if twin else [own_t, zero]
    rest = jnp.zeros((size.columns - 2 * size.cells, size.points), F32)
    full = from_across + jnp.concatenate(placed + [rest], axis=0)
    tail = jnp.where(iota((8, size.points), 0) == 0, 1.0, 0.0)
    return jnp.concatenate([full, tail], axis=0) * mass_row


def spread_of(size, tables):
    start = 2 * size.edges + size.cells
    return tables[start : start + 4 * size.edges, :]


SUBLANES = 8


def crm_kernel(size, levels, width, count, *refs):
    state_hbm, given = refs[0], refs[1 : 1 + count]
    new_ref, face_ref = refs[1 + count : 3 + count]
    held = refs[3 + count : 3 + 2 * count]
    state_ref, table_ref, wide_ref, out_buf, base_ref, inc_ref, change_ref = refs[
        3 + 2 * count : 10 + 2 * count
    ]
    state_sem, held_sem = refs[10 + 2 * count :]
    fields = state_ref.shape[0]
    steps = levels // SUBLANES
    per_lane = LANES // width
    full = (SUBLANES, LANES)
    lane = iota(full, 1)
    pair_lanes = 2 * LANES
    pairs = size.elements // 2

    def load(f):
        return pltpu.make_async_copy(state_hbm.at[f], state_ref.at[f], state_sem.at[f])

    small = [
        pltpu.make_async_copy(src, dst, held_sem.at[n])
        for n, (src, dst) in enumerate(zip(given, held))
    ]
    for copy in small:
        copy.start()
    for f in range(fields):
        load(f).start()
    table_ref[...] = jnp.zeros(table_ref.shape, F32)
    change_ref[...] = jnp.zeros(change_ref.shape, F32)
    base_ref[...] = jnp.zeros(base_ref.shape, F32)
    inc_ref[...] = jnp.zeros(inc_ref.shape, F32)
    for copy in small:
        copy.wait()
    first = 0
    for ref in held:
        rows, lanes = ref.shape
        table_ref[first : first + rows, 0:lanes] = ref[...].astype(F32)
        first += rows
    params = table_ref[...]

    def spread(ref, i):
        return ref[pl.ds(i, SUBLANES, stride=steps), :]

    eye = iota((levels, LANES), 0) == iota((levels, LANES), 1)
    mixz = jnp.broadcast_to(params[4:5, :], (levels, LANES))
    couple = jnp.sum(jnp.where(eye, mixz, 0.0), axis=1, keepdims=True)
    couple = jnp.where(iota((levels, 1), 0) < levels - 1, couple, 0.0)
    wide_ref[0, 0] = jnp.broadcast_to(couple, (levels, LANES))
    coupling = [spread(wide_ref.at[0, 0], i) for i in range(steps)]

    def vertical(a):
        above = a[1:] + [pltpu.roll(a[0], SUBLANES - 1, 0)]
        flux = [c * (u - v) for c, u, v in zip(coupling, above, a)]
        below = [pltpu.roll(flux[-1], 1, 0)] + flux[:-1]
        return [v + f - b for v, f, b in zip(a, flux, below)]

    level = [iota(full, 0) * steps + i for i in range(steps)]
    first = lane - lane % width
    east_lane = first + (lane + 1) % width
    west_lane = first + (lane + width - 1) % width

    def lanes_of(value, index):
        return jnp.take_along_axis(value, index, axis=1)

    def lanes_at(e, count=1):
        return pl.ds(pl.multiple_of(e * LANES, LANES), count * LANES)

    def widen(e, half):
        for f in range(fields):
            wide_ref[half, f] = state_ref[f, :, lanes_at(e)].astype(F32)

    def advance_element(e, half):
        here = lanes_of(params[0:SUBLANES, :], e * per_lane + lane // width)

        def row(r):
            return jnp.broadcast_to(here[r : r + 1, :], full)

        active, mix, drift, rate = row(0).astype(I32), row(1), row(2), row(3)
        centre, east_c, west_c = 1.0 - 2.0 * mix, mix - 0.5 * drift, mix + 0.5 * drift
        alive = [v < active for v in level]
        ice = [jnp.where(v, 0.15, 0.0) for v in alive]

        def transport(a):
            a = [
                centre * v + east_c * lanes_of(v, east_lane) + west_c * lanes_of(v, west_lane)
                for v in a
            ]
            return vertical(a)

        def keep(f):
            for i in range(steps):
                out_buf[half, f, pl.ds(i, SUBLANES, stride=steps), :] = cur[f][i]
            new_ref[f, :, lanes_at(e)] = out_buf[half, f].astype(BF16)

        cur = [[spread(wide_ref.at[half, f], i) for i in range(steps)] for f in range(fields)]
        changes = []
        for substep in range(NSUB):
            cur = [transport(a) for a in cur]
            if substep == NSUB - 1:
                for f in range(4, fields):
                    keep(f)
            conds, freezes = [], []
            for i in range(steps):
                t, qv, ql, qi = [cur[f][i] for f in range(4)]
                sat = jnp.exp2((0.3 * math.log2(math.e)) * t - 1.0)
                cond = jnp.where(alive[i], jnp.maximum(rate * (qv - sat), -ql), 0.0)
                ql = ql + cond
                t = t + 0.5 * cond
                freeze = ice[i] * ql * (1.0 - jnp.tanh(t))
                cur[0][i] = t + 0.1 * freeze
                cur[1][i] = qv - cond
                cur[2][i] = ql - freeze
                cur[3][i] = qi + freeze
                conds.append(cond)
                freezes.append(freeze)
            changes += conds + freezes
        for f in range(4):
            keep(f)
        for n, value in enumerate(changes):
            change_ref[n * SUBLANES : (n + 1) * SUBLANES, half * LANES : (half + 1) * LANES] = value

    cells = pair_lanes // width
    group = iota((pair_lanes, LANES), 0) // width == iota((pair_lanes, LANES), 1) % cells
    total = jnp.where(group, 1.0, 0.0).astype(BF16)

    def set_sums(ref, p, sums):
        mine = jnp.broadcast_to(lane[0:1, :] // cells == p, sums.shape)
        ref[...] = jnp.where(mine, sums, ref[...])

    def sum_changes(p):
        change = change_ref[...]
        high = change.astype(BF16)
        low = (change - high.astype(F32)).astype(BF16)
        set_sums(inc_ref, p, dot_nn(high, total, None) + dot_nn(low, total, None))

    def pair(p, carry):
        sum_changes(p - 1)
        widen(2 * p + 1, 1)
        advance_element(2 * p, 0)
        for f in range(fields):
            set_sums(base_ref.at[f], p, dot_nn(state_ref[f, :, lanes_at(2 * p, 2)], total, None))
        widen(jnp.minimum(2 * p + 2, size.elements - 1), 0)
        advance_element(2 * p + 1, 1)
        return carry

    parity = lax.axis_index("tile") % 2
    slots_row = flat_row(params[6:10, 0 : size.elements])
    codes_row = flat_row(params[10:14, 0 : size.elements])
    edges = Edges(size, slots_row.astype(I32), codes_row.astype(I32), parity)
    slot = side_slots(size, edges.side, edges.flat)
    rows = 2 * size.raw
    place = jnp.where(edges.side >= 0, size.cells + edges.side * size.raw + 2 * slot, -8)
    put = jnp.concatenate([place, place + 1], axis=1)
    cell = jnp.concatenate(
        [4 * edges.e + edge_cell(edges.k, m) for m in range(2)], axis=1
    )
    select = jnp.where(iota((LANES, 2 * size.edges), 0) == put, 1.0, 0.0)
    cell = jnp.broadcast_to(cell.astype(F32), (SUBLANES, 2 * size.edges))
    picked = dot_nt(cell, select, None).astype(I32)
    source = jnp.where(lane < size.cells, lane, picked)

    for f in range(fields):
        load(f).wait()
    widen(0, 0)
    lax.fori_loop(0, pairs, pair, 0)
    sum_changes(pairs - 1)

    def change_of(n):
        return [
            inc_ref[(n * steps + i) * SUBLANES : (n * steps + i + 1) * SUBLANES, :]
            for i in range(steps)
        ]

    parts = [[change_of(2 * n), change_of(2 * n + 1)] for n in range(NSUB)]
    scale = PER_TIME / width
    columns = []
    for f in range(fields):
        start = [spread(base_ref.at[f], i) for i in range(steps)]
        mean = start
        for cond, freeze in parts:
            mean = vertical(mean)
            if f == 0:
                mean = [v + 0.5 * c + 0.1 * z for v, c, z in zip(mean, cond, freeze)]
            elif f == 1:
                mean = [v - c for v, c in zip(mean, cond)]
            elif f == 2:
                mean = [v + c - z for v, c, z in zip(mean, cond, freeze)]
            elif f == 3:
                mean = [v + z for v, z in zip(mean, freeze)]
        columns += [lanes_of(scale * (v - s), source) for v, s in zip(mean, start)]
    columns.append(jnp.zeros((size.wide - size.flat, LANES), F32))
    tendency = jnp.concatenate(columns, axis=0)
    base = size.cells + rows
    face_ref[0:base, :] = tendency.T[0:base, :]
    face_ref[base:, :] = jnp.zeros((SUBLANES, size.wide), F32)
    face_ref[base : base + 1, 0 : size.edges] = slots_row
    face_ref[base + 1 : base + 2, 0 : size.edges] = codes_row
    face_ref[base + 2 : base + 3, 0 : size.points] = params[5:6, 0 : size.points]


def face_edges(size, face_ref, parity):
    base = size.cells + 2 * size.raw
    slots_row = face_ref[base : base + 1, 0 : size.edges].astype(I32)
    codes_row = face_ref[base + 1 : base + 2, 0 : size.edges].astype(I32)
    mass_row = face_ref[base + 2 : base + 3, 0 : size.points]
    return Edges(size, slots_row, codes_row, parity), mass_row


def weights_kernel(size, own_ref, table_ref, part_ref):
    parity = lax.axis_index("tile") % 2
    edges, mass_row = face_edges(size, own_ref, parity)
    tables = table_ref[...]
    slot_far = side_slots(size, edges.side, edges.other_flat)
    oper_t = operator_t(
        size, tables, gather_matrix_t(size, edges, slot_far, 0), mass_row, False
    )
    slot = side_slots(size, edges.side, edges.flat)
    rows = 2 * size.part
    first = jnp.where(edges.side >= 0, edges.side * size.part + 4 * slot, -8)
    put = jnp.concatenate([first + t for t in range(4)], axis=1)
    select = jnp.where(iota((rows, 4 * size.edges), 0) == put, 1.0, 0.0)
    points = dot_nn(select, spread_of(size, tables), None)
    part = dot_nt(points, oper_t)
    n = size.elements
    both = jnp.zeros((1, n), I32)
    hits = []
    for s in range(2):
        hit = jnp.where(edges.side == s, 1, 0)
        total = hit[:, 0:n]
        for k in range(1, 4):
            total = total + hit[:, k * n : (k + 1) * n]
        hits.append(total)
    both = jnp.where(jnp.logical_and(hits[0] > 0, hits[1] > 0), 1.0, 0.0)
    flag = jnp.max(both)
    part_ref[:, 0 : size.ops] = part
    part_ref[:, size.ops :] = jnp.full((rows, LANES - size.ops), flag, F32)


def message_kernel(size, own_ref, twin_ref, part_ref, even_ref, odd_ref):
    cells = jnp.concatenate([own_ref[0 : size.cells, :], twin_ref[0 : size.cells, :]], axis=0)
    weights = stack_left(part_ref[:, 0 : 2 * size.cells], 1)
    part = dot_nn(weights, stack_right(cells, 0), None)
    lane = iota((2 * size.part, size.wide), 1)
    part = jnp.where(lane == size.flat, part_ref[:, size.columns : size.columns + 1], part)
    part = jnp.where(lane == size.flat + 1, part_ref[:, size.ops : size.ops + 1], part)
    for s, ref in enumerate((even_ref, odd_ref)):
        first = size.cells + s * size.raw
        ref[0 : size.raw, :] = own_ref[first : first + size.raw, :]
        ref[size.raw : 2 * size.raw, :] = twin_ref[first : first + size.raw, :]
        ref[2 * size.raw :, :] = part[s * size.part : (s + 1) * size.part, :]


def inner_kernel(
    size, table_ref, own_ref, twin_ref, state_ref, sum_ref, near_ref, matrix_ref, new_ref, sem
):
    save = pltpu.make_async_copy(state_ref, new_ref, sem)
    save.start()
    parity = lax.axis_index("tile") % 2
    tables = table_ref[...]
    own, own_mass = face_edges(size, own_ref, parity)
    twin, twin_mass = face_edges(size, twin_ref, parity)
    own_slot = side_slots(size, own.side, own.other_flat)
    twin_slot = side_slots(size, twin.side, twin.other_flat)
    oper = jnp.concatenate(
        [
            operator_t(size, tables, gather_matrix_t(size, own, own_slot, 0), own_mass, False),
            operator_t(size, tables, gather_matrix_t(size, twin, twin_slot, 1), twin_mass, True),
        ],
        axis=1,
    )
    far = 2 * size.points
    targets = []
    for t in range(4):
        tt = jnp.where(own.turned == 1, 3 - t, t)
        point = 16 * own.place + edge_point(own.other_k, tt)
        local = jnp.where(own.source == 0, 0, size.points) + point
        targets.append(
            jnp.where(own.side >= 0, far + own.side * size.part + 4 * own_slot + tt, local)
        )
    target = jnp.concatenate(targets, axis=1)
    rows = far + 2 * size.part
    partner_t = jnp.where(iota((rows, 4 * size.edges), 0) == target, 1.0, 0.0)
    assemble_t = dot_nn(partner_t, spread_of(size, tables), None)
    eye = jnp.where(iota((far, size.points), 0) == iota((far, size.points), 1), 1.0, 0.0)
    total_t = dot_nn(oper, assemble_t[0:far, :] + eye)
    cells = 2 * size.cells
    matrix_ref[0 : 4 * size.raw, :] = total_t[cells : size.columns, :]
    matrix_ref[4 * size.raw : 4 * size.raw + 2 * size.part, :] = assemble_t[far:, :]
    matrix_ref[4 * size.raw + 2 * size.part :, :] = total_t[size.columns :, :]
    chip = jnp.concatenate([own_ref[0 : size.cells, :], twin_ref[0 : size.cells, :]], axis=0)
    sum_ref[...] = dot_tn(chip[:, 0 : size.flat], total_t[0:cells, :])
    side_slot = jnp.where(own.side >= 0, own.side * BLK_R + own_slot, -1)
    match = jnp.broadcast_to(twice(side_slot), (2 * size.part, 2 * size.edges)) == (
        iota((2 * size.part, 2 * size.edges), 0) // 4
    )
    t_of = iota((2 * size.part, 2 * size.edges), 0) % 4
    m_of = iota((2 * size.part, 2 * size.edges), 1) // size.edges
    weight = jnp.zeros(match.shape, F32)
    for t in range(4):
        for m in range(2):
            here = jnp.logical_and(t_of == t, m_of == m)
            weight = jnp.where(here, edge_weight(t, m), weight)
    weight = jnp.where(match, weight, 0.0)
    cell = jnp.concatenate(
        [
            4 * own.e + edge_cell(own.k, jnp.where(own.turned == 1, 1 - m, m))
            for m in range(2)
        ],
        axis=1,
    )
    cell_t = jnp.where(iota((size.cells, 2 * size.edges), 0) == cell, 1.0, 0.0)
    near_ref[...] = dot_nn(dot_nt(weight, cell_t), own_ref[0 : size.cells, :])
    save.wait()


def final_kernel(
    size,
    levels,
    even_ref,
    odd_ref,
    sum_ref,
    near_ref,
    matrix_ref,
    part_ref,
    out_ref,
    keep_ref,
    flag_ref,
):
    raw = 2 * size.raw
    mine = part_ref[0:1, size.ops : size.ops + 1]
    others = [ref[raw : raw + 1, size.flat + 1 : size.flat + 2] for ref in (even_ref, odd_ref)]
    flag = jnp.where(mine + others[0] + others[1] > 0.0, 1.0, 0.0)
    flag_ref[0, 0] = jnp.sum(flag).astype(I32)
    mass = jnp.concatenate(
        [ref[raw:, size.flat : size.flat + 1] for ref in (even_ref, odd_ref)], axis=0
    )
    part = jnp.concatenate([even_ref[raw:, :], odd_ref[raw:, :]], axis=0)
    part = part + mass * near_ref[...]
    rows = jnp.concatenate([even_ref[0:raw, :], odd_ref[0:raw, :], part], axis=0)
    n = 2 * raw + 2 * size.part
    side = matrix_ref[2 * raw : n, :]
    mass_sum = matrix_ref[n : n + 1, :] + jnp.sum(side * mass, axis=0, keepdims=True)
    keep_ref[...] = jnp.broadcast_to(mass_sum, (8, size.points))
    wide = dot_tn(stack_left(rows, 0), stack_right(matrix_ref[0:n, :], 0), None)
    total = sum_ref[...] + wide[0 : size.flat, :]
    total = total / mass_sum
    steps = levels // SUBLANES
    for f in range(size.flat // levels):
        for i in range(steps):
            row = (f * steps + i) * SUBLANES
            out_ref[pl.ds(f * levels + i, SUBLANES, stride=steps), :] = total[row : row + SUBLANES, :]


VMEM = pl.BlockSpec(memory_space=pltpu.VMEM)
SMEM = pl.BlockSpec(memory_space=pltpu.SMEM)
HBM = pl.BlockSpec(memory_space=pltpu.HBM)


def call(body, name, outs, ins, in_specs=None, out_specs=None, scratch=(), limit=8):
    return pl.pallas_call(
        body,
        out_shape=outs,
        in_specs=in_specs or [VMEM] * len(ins),
        out_specs=out_specs or [VMEM] * len(outs),
        scratch_shapes=scratch,
        compiler_params=pltpu.CompilerParams(vmem_limit_bytes=limit * 1024 * 1024),
        name=name,
    )(*ins)


def shape_of(*dims):
    return jax.ShapeDtypeStruct(dims, F32)


def advance(size, crm_state, params):
    fields, levels, lanes = crm_state.shape
    width = lanes // size.cells
    block = pltpu.VMEM((2, fields, levels, LANES), F32)
    params = [value.reshape(-1, value.shape[-1]) for value in params]
    rows = sum(value.shape[0] for value in params)
    ins = [pltpu.with_memory_space_constraint(value, pltpu.HBM) for value in (crm_state, *params)]
    return call(
        functools.partial(crm_kernel, size, levels, width, len(params)),
        "advance",
        [
            pltpu.VMEM(crm_state.shape, BF16),
            pltpu.VMEM((size.face_rows, size.wide), F32),
        ],
        ins,
        in_specs=[HBM] * len(ins),
        scratch=[pltpu.VMEM(value.shape, value.dtype) for value in params]
        + [
            pltpu.VMEM(crm_state.shape, BF16),
            pltpu.VMEM((-(-rows // SUBLANES) * SUBLANES, LANES), F32),
            block,
            block,
            pltpu.VMEM((fields, levels, LANES), F32),
            pltpu.VMEM((2 * NSUB * levels, LANES), F32),
            pltpu.VMEM((2 * NSUB * levels, 2 * LANES), F32),
            pltpu.SemaphoreType.DMA((fields,)),
            pltpu.SemaphoreType.DMA((len(params),)),
        ],
        limit=16,
    )


def swap_pairs(odd):
    tiles = lax.axis_size("tile")
    pairs = []
    for t in range(tiles):
        up = (t % 2 == 0) != odd
        pairs.append((t, (t + 1 if up else t - 1) % tiles))
    return pairs


def swap(value, odd):
    return lax.ppermute(value, "tile", swap_pairs(odd))


def shift(value, axis, steps):
    count = lax.axis_size(axis)
    return lax.ppermute(value, axis, [(s, (s + steps) % count) for s in range(count)])


def assemble_pair(size, levels, state, face):
    tables = jnp.asarray(constant_tables(size))
    twin = shift(face, "face", 1)
    (part,) = call(
        functools.partial(weights_kernel, size),
        "weights",
        [shape_of(2 * size.part, LANES)],
        [face, tables],
    )
    message = shape_of(size.tile_rows, size.wide)
    even, odd = call(
        functools.partial(message_kernel, size), "message", [message] * 2, [face, twin, part]
    )
    odd_in = swap(odd, True)
    even_in = swap(even, False)
    extra = 4 * size.raw + 2 * size.part
    inner, near, matrix, new_state = call(
        functools.partial(inner_kernel, size),
        "inner",
        [
            shape_of(size.flat, size.points),
            shape_of(2 * size.part, size.wide),
            shape_of(extra + 8, size.points),
            pltpu.HBM(state.shape, state.dtype),
        ],
        [tables, face, twin, pltpu.with_memory_space_constraint(state, pltpu.VMEM)],
        out_specs=[VMEM, VMEM, VMEM, HBM],
        scratch=[pltpu.SemaphoreType.DMA],
    )
    out, keep, flag = call(
        functools.partial(final_kernel, size, levels),
        "final",
        [
            pltpu.VMEM((size.flat, size.points), F32),
            shape_of(8, size.points),
            pltpu.SMEM((1, 1), I32),
        ],
        [even_in, odd_in, inner, near, matrix, part],
        out_specs=[VMEM, VMEM, SMEM],
    )
    return new_state, (out, part, keep, matrix, even_in, odd_in, flag)


def one_of(index, branches, *operands):
    whole = jax.make_jaxpr(lambda i, *rest: lax.switch(i, branches, *rest))(index, *operands)
    last = whole.jaxpr.eqns[-1]
    return last.primitive.bind(index, *operands, **last.params)[0]


def second_exchange(size, levels, out, part, keep, matrix, even_in, odd_in, flag):
    raw = 2 * size.raw

    def add(s, value, part, keep, matrix, even_in, odd_in):
        source = (odd_in, even_in)[s]
        first = 2 * size.cells + raw * (1 - s)
        weights = part[s * size.part : (s + 1) * size.part, first : first + raw]
        side = matrix[2 * raw + s * size.part : 2 * raw + (s + 1) * size.part, :]
        sent = jnp.dot(weights, source[0:raw, 0 : size.flat], precision=HI)
        got = swap(sent, s == 1)
        more = jnp.dot(got.T, side, precision=HI) / keep[0:1, :]
        more = more.reshape(-1, levels // SUBLANES, SUBLANES, size.points)
        return value + more.transpose(0, 2, 1, 3).reshape(value.shape)

    def none(value, *rest):
        return value

    def some(value, *rest):
        mine = rest[0][0, size.ops]
        for s, received in ((0, rest[3]), (1, rest[4])):
            other = received[raw, size.flat + 1]
            value = lax.cond(
                mine + other > 0.0, functools.partial(add, s), none, value, *rest
            )
        return value

    operands = (out, part, keep, matrix, even_in, odd_in)
    return one_of(flag[0, 0], (none, some), *operands)


def oriented(edge_lists):
    rows = []
    for code in range(8):
        side = list(edge_lists[code // 2])
        rows.append(side[::-1] if code % 2 == 1 else side)
    return np.array(rows, np.int32)


def collect(value, slots):
    pieces = [value]
    for axis, steps in (("tile", 1), ("tile", -1), ("face", 1), ("face", -1)):
        pieces.append(shift(value, axis, steps))
    return jnp.concatenate(pieces, axis=0), slots


def assemble_any(size, levels, face, masses, slots, codes):
    elements = size.elements
    cells = face[0 : size.cells, 0 : size.flat].reshape(elements, 4, size.flat)
    pool, rows = collect(cells, slots)
    pick = jnp.take(jnp.asarray(oriented(CELL_EDGE)), codes, axis=0)
    index = (rows[:, :, None] * 4 + pick).transpose(1, 0, 2).reshape(-1)
    across = jnp.take(pool.reshape(-1, size.flat), index, axis=0)
    stacked = jnp.concatenate([cells, across.reshape(elements, 8, size.flat)], axis=1)
    points = jnp.einsum("ecz,pc->epz", stacked, jnp.asarray(remap_matrix()), precision=HI)
    masses = masses.reshape(elements, 16)
    numerator, denominator = points * masses[:, :, None], masses
    weighted, rows = collect(numerator, slots)
    mass_pool, _ = collect(masses, slots)
    pick = jnp.take(jnp.asarray(oriented(GLL_EDGE)), codes, axis=0)
    for k in range(4):
        index = (rows[k][:, None] * 16 + pick[k]).reshape(-1)
        got = jnp.take(weighted.reshape(-1, size.flat), index, axis=0)
        numerator = numerator.at[:, GLL_EDGE[k]].add(got.reshape(elements, 4, size.flat))
        got = jnp.take(mass_pool.reshape(-1), index)
        denominator = denominator.at[:, GLL_EDGE[k]].add(got.reshape(elements, 4))
    ratio = (numerator / denominator[:, :, None]).reshape(size.points, size.flat)
    ratio = ratio.reshape(size.points, -1, levels // SUBLANES, SUBLANES)
    return ratio.transpose(1, 3, 2, 0).reshape(size.flat, size.points)


def local(
    crm_state,
    active_levels,
    mix_x,
    drift_speed,
    cond_rate,
    mix_z,
    point_mass,
    neighbor_slots,
    edge_codes,
):
    fields, levels, _ = crm_state.shape
    size = Sizes(neighbor_slots.shape[1], fields * levels)
    params = (
        active_levels,
        mix_x,
        drift_speed,
        cond_rate,
        mix_z,
        point_mass,
        neighbor_slots,
        edge_codes,
    )
    state, face = advance(size, crm_state, params)
    tiles = lax.axis_size("tile")
    if lax.axis_size("face") == 2 and tiles % 2 == 0 and tiles > 2:
        new_state, results = assemble_pair(size, levels, state, face)
        out = second_exchange(size, levels, *results)
    else:
        new_state = state
        out = assemble_any(size, levels, face, point_mass, neighbor_slots, edge_codes)
    return (new_state, out.reshape(fields, levels, size.points))


def solution(mesh):
    in_specs = (
        P(None, None, ("face", "tile")),
        P(("face", "tile")),
        P(("face", "tile")),
        P(("face", "tile")),
        P(("face", "tile")),
        P(),
        P(("face", "tile")),
        P(None, ("face", "tile")),
        P(None, ("face", "tile")),
    )
    out_specs = (P(None, None, ("face", "tile")), P(None, None, ("face", "tile")))
    return jax.shard_map(local, mesh=mesh, in_specs=in_specs, out_specs=out_specs, check_vma=False)
```

```python
import functools
import math

import jax
import jax.numpy as jnp
import numpy as np
from jax import lax
from jax.experimental import pallas as pl
from jax.experimental.pallas import tpu as pltpu
from jax.sharding import PartitionSpec as P

NSUB = 2
BLK_R = 4
BLK_C = 2
PER_TIME = 10.0
LANES = 128
HI = lax.Precision.HIGHEST
F32 = jnp.float32
BF16 = jnp.bfloat16
I32 = jnp.int32

CELL_EDGE = [[0, 1], [1, 3], [2, 3], [0, 2]]
GLL_EDGE = [[0, 1, 2, 3], [3, 7, 11, 15], [12, 13, 14, 15], [0, 4, 8, 12]]


def lagrange(q, z):
    centres = [-1.5, -0.5, 0.5, 1.5]
    product = 1.0
    for r in range(4):
        if r != q:
            product = product * (z - centres[r]) / (centres[q] - centres[r])
    return product


def linear_weight(j, z):
    return 0.5 - z if j == 0 else 0.5 + z


GLL_NODES = [-1.0, -1.0 / math.sqrt(5.0), 1.0 / math.sqrt(5.0), 1.0]


def remap_matrix():
    matrix = [[0.0 for column in range(12)] for row in range(16)]
    for b in range(4):
        for a in range(4):
            p = 4 * b + a
            x = GLL_NODES[a]
            y = GLL_NODES[b]
            for j in range(2):
                for i in range(2):
                    matrix[p][2 * j + i] += 0.5 * linear_weight(j, y) * lagrange(
                        1 + i, x
                    ) + 0.5 * linear_weight(i, x) * lagrange(1 + j, y)
            for m in range(2):
                matrix[p][4 + 6 + m] += 0.5 * linear_weight(m, y) * lagrange(0, x)
                matrix[p][4 + 2 + m] += 0.5 * linear_weight(m, y) * lagrange(3, x)
                matrix[p][4 + 0 + m] += 0.5 * linear_weight(m, x) * lagrange(0, y)
                matrix[p][4 + 4 + m] += 0.5 * linear_weight(m, x) * lagrange(3, y)
    return np.array(matrix, np.float32)


class Sizes:
    def __init__(self, elements, flat_len):
        self.elements = elements
        self.edges = 4 * elements
        self.cells = 4 * elements
        self.points = 16 * elements
        self.raw = 2 * BLK_R
        self.part = 4 * BLK_R
        self.flat = flat_len
        self.wide = -(-(flat_len + 2) // LANES) * LANES
        self.columns = 2 * self.cells + 4 * self.raw
        self.ops = self.columns + 8
        self.face_rows = self.cells + 2 * self.raw + 8
        self.tile_rows = 2 * self.raw + self.part


def constant_tables(size):
    matrix = remap_matrix()
    across_t = np.zeros((2 * size.edges, size.points), np.float32)
    own_t = np.zeros((size.cells, size.points), np.float32)
    spread_t = np.zeros((4 * size.edges, size.points), np.float32)
    for e in range(size.elements):
        for p in range(16):
            for c in range(4):
                own_t[4 * e + c, 16 * e + p] = matrix[p][c]
            for k in range(4):
                for m in range(2):
                    row = m * size.edges + k * size.elements + e
                    across_t[row, 16 * e + p] = matrix[p][4 + 2 * k + m]
        for k in range(4):
            for t in range(4):
                row = t * size.edges + k * size.elements + e
                spread_t[row, 16 * e + GLL_EDGE[k][t]] = 1.0
    return np.concatenate([across_t, own_t, spread_t], axis=0)


def edge_weight(t, m):
    return 0.5 * linear_weight(m, GLL_NODES[t]) * lagrange(0, -1.0)


def iota(shape, dim):
    return lax.broadcasted_iota(I32, shape, dim)


def dot_nn(a, b, precision=HI):
    return lax.dot_general(
        a, b, (((1,), (0,)), ((), ())), precision=precision, preferred_element_type=F32
    )


def dot_nt(a, b, precision=HI):
    return lax.dot_general(
        a, b, (((1,), (1,)), ((), ())), precision=precision, preferred_element_type=F32
    )


def dot_tn(a, b, precision=HI):
    return lax.dot_general(
        a, b, (((0,), (0,)), ((), ())), precision=precision, preferred_element_type=F32
    )


def split(value):
    high = value.astype(BF16)
    return high, (value - high.astype(F32)).astype(BF16)


def stack_left(value, axis):
    high, low = split(value)
    return jnp.concatenate([high, low, high], axis=axis)


def stack_right(value, axis):
    high, low = split(value)
    return jnp.concatenate([high, high, low], axis=axis)


def flat_row(table):
    return jnp.concatenate([table[k : k + 1, :] for k in range(4)], axis=1)


def twice(row):
    return jnp.concatenate([row, row], axis=1)


def side_slots(size, side, order):
    n = size.edges
    key = jnp.where(side >= 0, side * 2 * n + order, 8 * n)
    eye = iota((n, n), 0) == iota((n, n), 1)
    wide = jnp.broadcast_to(key.astype(F32), (n, n))
    column = jnp.sum(jnp.where(eye, wide, 0.0), axis=1, keepdims=True)
    floor = jnp.broadcast_to((side * 2 * n).astype(F32), (n, n))
    lower = jnp.logical_and(column < wide, column >= floor)
    count = jnp.sum(jnp.where(lower, 1.0, 0.0), axis=0, keepdims=True).astype(I32)
    return jnp.where(side >= 0, count, 0)


def edge_cell(k, m):
    odd = k & 1
    base = jnp.where(k == 2, 2, odd * jnp.where(k == 1, 1, 0))
    return base + m * (1 + odd)


def edge_point(k, t):
    odd = k & 1
    base = jnp.where(k == 2, 12, jnp.where(k == 1, 3, 0))
    return base + t * (1 + 3 * odd)


class Edges:
    def __init__(self, size, slots_row, codes_row, parity):
        n = size.edges
        flat = iota((1, n), 1)
        self.k = flat // size.elements
        self.e = flat % size.elements
        self.source = slots_row // size.elements
        self.place = slots_row % size.elements
        self.other_k = codes_row // 2
        self.turned = codes_row % 2
        self.side = jnp.where(
            self.source == 2 - parity, 0, jnp.where(self.source == 1 + parity, 1, -1)
        )
        self.flat = flat
        self.other_flat = self.other_k * size.elements + self.place


def gather_matrix_t(size, edges, slot, twin):
    cells, raw = size.cells, size.raw
    rows = []
    for m in range(2):
        mm = jnp.where(edges.turned == 1, 1 - m, m)
        cell = 4 * edges.place + edge_cell(edges.other_k, mm)
        local = jnp.where(edges.source == 0, cells * twin, cells * (1 - twin)) + cell
        far = 2 * cells + 2 * raw * edges.side + raw * twin + 2 * slot + mm
        rows.append(jnp.where(edges.side >= 0, far, local))
    target = jnp.concatenate(rows, axis=1)
    return jnp.where(iota((size.columns, 2 * size.edges), 0) == target, 1.0, 0.0)


def operator_t(size, tables, gather_t, mass_row, twin):
    across_t = tables[0 : 2 * size.edges, :]
    own_t = tables[2 * size.edges : 2 * size.edges + size.cells, :]
    from_across = dot_nn(gather_t, across_t)
    zero = jnp.zeros((size.cells, size.points), F32)
    placed = [zero, own_t] if twin else [own_t, zero]
    rest = jnp.zeros((size.columns - 2 * size.cells, size.points), F32)
    full = from_across + jnp.concatenate(placed + [rest], axis=0)
    tail = jnp.where(iota((8, size.points), 0) == 0, 1.0, 0.0)
    return jnp.concatenate([full, tail], axis=0) * mass_row


def spread_of(size, tables):
    start = 2 * size.edges + size.cells
    return tables[start : start + 4 * size.edges, :]


SUBLANES = 8


def crm_kernel(size, levels, width, count, *refs):
    state_hbm, given = refs[0], refs[1 : 1 + count]
    new_ref, face_ref = refs[1 + count : 3 + count]
    held = refs[3 + count : 3 + 2 * count]
    state_ref, table_ref, wide_ref, out_buf, base_ref, inc_ref, change_ref = refs[
        3 + 2 * count : 10 + 2 * count
    ]
    state_sem, held_sem = refs[10 + 2 * count :]
    fields = state_ref.shape[0]
    steps = levels // SUBLANES
    per_lane = LANES // width
    full = (SUBLANES, LANES)
    lane = iota(full, 1)
    pair_lanes = 2 * LANES
    pairs = size.elements // 2

    def load(f):
        return pltpu.make_async_copy(state_hbm.at[f], state_ref.at[f], state_sem.at[f])

    small = [
        pltpu.make_async_copy(src, dst, held_sem.at[n])
        for n, (src, dst) in enumerate(zip(given, held))
    ]
    for copy in small:
        copy.start()
    for f in range(fields):
        load(f).start()
    table_ref[...] = jnp.zeros(table_ref.shape, F32)
    change_ref[...] = jnp.zeros(change_ref.shape, F32)
    base_ref[...] = jnp.zeros(base_ref.shape, F32)
    inc_ref[...] = jnp.zeros(inc_ref.shape, F32)
    for copy in small:
        copy.wait()
    first = 0
    for ref in held:
        rows, lanes = ref.shape
        table_ref[first : first + rows, 0:lanes] = ref[...].astype(F32)
        first += rows
    params = table_ref[...]

    def spread(ref, i):
        return ref[pl.ds(i, SUBLANES, stride=steps), :]

    eye = iota((levels, LANES), 0) == iota((levels, LANES), 1)
    mixz = jnp.broadcast_to(params[4:5, :], (levels, LANES))
    couple = jnp.sum(jnp.where(eye, mixz, 0.0), axis=1, keepdims=True)
    couple = jnp.where(iota((levels, 1), 0) < levels - 1, couple, 0.0)
    wide_ref[0, 0] = jnp.broadcast_to(couple, (levels, LANES))
    coupling = [spread(wide_ref.at[0, 0], i) for i in range(steps)]

    def vertical(a):
        above = a[1:] + [pltpu.roll(a[0], SUBLANES - 1, 0)]
        flux = [c * (u - v) for c, u, v in zip(coupling, above, a)]
        below = [pltpu.roll(flux[-1], 1, 0)] + flux[:-1]
        return [v + f - b for v, f, b in zip(a, flux, below)]

    level = [iota(full, 0) * steps + i for i in range(steps)]
    first = lane - lane % width
    east_lane = first + (lane + 1) % width
    west_lane = first + (lane + width - 1) % width

    def lanes_of(value, index):
        return jnp.take_along_axis(value, index, axis=1)

    def lanes_at(e, count=1):
        return pl.ds(pl.multiple_of(e * LANES, LANES), count * LANES)

    def column_rows(e):
        here = lanes_of(params[0:SUBLANES, :], e * per_lane + lane // width)
        active, mix, drift, rate = [
            jnp.broadcast_to(here[r : r + 1, :], full) for r in range(4)
        ]
        return active, rate, (1.0 - 2.0 * mix, mix - 0.5 * drift, mix + 0.5 * drift)

    def transport(value, weights):
        centre, east_c, west_c = weights
        east, west = lanes_of(value, east_lane), lanes_of(value, west_lane)
        return centre * value + east_c * east + west_c * west

    def transport_first(e, half):
        _, _, weights = column_rows(e)
        for f in range(fields):
            value = state_ref[f, :, lanes_at(e)].astype(F32)
            for i in range(steps):
                rows = slice(i * SUBLANES, (i + 1) * SUBLANES)
                wide_ref[half, f, rows, :] = transport(value[rows, :], weights)

    def advance_element(e, half):
        active, rate, weights = column_rows(e)
        active = active.astype(I32)
        alive = [v < active for v in level]
        ice = [jnp.where(v, 0.15, 0.0) for v in alive]

        def keep(f):
            for i in range(steps):
                out_buf[half, f, pl.ds(i, SUBLANES, stride=steps), :] = cur[f][i]
            new_ref[f, :, lanes_at(e)] = out_buf[half, f].astype(BF16)

        cur = [[spread(wide_ref.at[half, f], i) for i in range(steps)] for f in range(fields)]
        changes = []
        for substep in range(NSUB):
            if substep > 0:
                cur = [[transport(v, weights) for v in a] for a in cur]
            cur = [vertical(a) for a in cur]
            if substep == NSUB - 1:
                for f in range(4, fields):
                    keep(f)
            conds, freezes = [], []
            for i in range(steps):
                t, qv, ql, qi = [cur[f][i] for f in range(4)]
                sat = jnp.exp2((0.3 * math.log2(math.e)) * t - 1.0)
                cond = jnp.where(alive[i], jnp.maximum(rate * (qv - sat), -ql), 0.0)
                ql = ql + cond
                t = t + 0.5 * cond
                freeze = ice[i] * ql * (1.0 - jnp.tanh(t))
                cur[0][i] = t + 0.1 * freeze
                cur[1][i] = qv - cond
                cur[2][i] = ql - freeze
                cur[3][i] = qi + freeze
                conds.append(cond)
                freezes.append(freeze)
            changes += conds + freezes
        for f in range(4):
            keep(f)
        for n, value in enumerate(changes):
            change_ref[n * SUBLANES : (n + 1) * SUBLANES, half * LANES : (half + 1) * LANES] = value

    cells = pair_lanes // width
    group = iota((pair_lanes, LANES), 0) // width == iota((pair_lanes, LANES), 1) % cells
    total = jnp.where(group, 1.0, 0.0).astype(BF16)

    def set_sums(ref, p, sums):
        mine = jnp.broadcast_to(lane[0:1, :] // cells == p, sums.shape)
        ref[...] = jnp.where(mine, sums, ref[...])

    def sum_changes(p):
        change = change_ref[...]
        high = change.astype(BF16)
        low = (change - high.astype(F32)).astype(BF16)
        set_sums(inc_ref, p, dot_nn(high, total, None) + dot_nn(low, total, None))

    def pair(p, carry):
        sum_changes(p - 1)
        transport_first(2 * p + 1, 1)
        advance_element(2 * p, 0)
        for f in range(fields):
            set_sums(base_ref.at[f], p, dot_nn(state_ref[f, :, lanes_at(2 * p, 2)], total, None))
        transport_first(jnp.minimum(2 * p + 2, size.elements - 1), 0)
        advance_element(2 * p + 1, 1)
        return carry

    for f in range(fields):
        load(f).wait()
    transport_first(0, 0)
    lax.fori_loop(0, pairs, pair, 0)
    sum_changes(pairs - 1)

    def change_of(n):
        return [
            inc_ref[(n * steps + i) * SUBLANES : (n * steps + i + 1) * SUBLANES, :]
            for i in range(steps)
        ]

    parts = [[change_of(2 * n), change_of(2 * n + 1)] for n in range(NSUB)]
    parity = lax.axis_index("tile") % 2
    slots_row = flat_row(params[6:10, 0 : size.elements])
    codes_row = flat_row(params[10:14, 0 : size.elements])
    edges = Edges(size, slots_row.astype(I32), codes_row.astype(I32), parity)
    slot = side_slots(size, edges.side, edges.flat)
    rows = 2 * size.raw
    place = jnp.where(edges.side >= 0, size.cells + edges.side * size.raw + 2 * slot, -8)
    put = jnp.concatenate([place, place + 1], axis=1)
    cell = jnp.concatenate(
        [4 * edges.e + edge_cell(edges.k, m) for m in range(2)], axis=1
    )
    select = jnp.where(iota((LANES, 2 * size.edges), 0) == put, 1.0, 0.0)
    cell = jnp.broadcast_to(cell.astype(F32), (SUBLANES, 2 * size.edges))
    picked = dot_nt(cell, select, None).astype(I32)
    source = jnp.where(lane < size.cells, lane, picked)

    scale = PER_TIME / width
    columns = []
    for f in range(fields):
        start = [spread(base_ref.at[f], i) for i in range(steps)]
        mean = start
        for cond, freeze in parts:
            mean = vertical(mean)
            if f == 0:
                mean = [v + 0.5 * c + 0.1 * z for v, c, z in zip(mean, cond, freeze)]
            elif f == 1:
                mean = [v - c for v, c in zip(mean, cond)]
            elif f == 2:
                mean = [v + c - z for v, c, z in zip(mean, cond, freeze)]
            elif f == 3:
                mean = [v + z for v, z in zip(mean, freeze)]
        columns += [lanes_of(scale * (v - s), source) for v, s in zip(mean, start)]
    columns.append(jnp.zeros((size.wide - size.flat, LANES), F32))
    tendency = jnp.concatenate(columns, axis=0)
    base = size.cells + rows
    face_ref[0:base, :] = tendency.T[0:base, :]
    face_ref[base:, :] = jnp.zeros((SUBLANES, size.wide), F32)
    face_ref[base : base + 1, 0 : size.edges] = slots_row
    face_ref[base + 1 : base + 2, 0 : size.edges] = codes_row
    face_ref[base + 2 : base + 3, 0 : size.points] = params[5:6, 0 : size.points]


def face_edges(size, face_ref, parity):
    base = size.cells + 2 * size.raw
    slots_row = face_ref[base : base + 1, 0 : size.edges].astype(I32)
    codes_row = face_ref[base + 1 : base + 2, 0 : size.edges].astype(I32)
    mass_row = face_ref[base + 2 : base + 3, 0 : size.points]
    return Edges(size, slots_row, codes_row, parity), mass_row


def weights_kernel(size, own_ref, table_ref, part_ref):
    parity = lax.axis_index("tile") % 2
    edges, mass_row = face_edges(size, own_ref, parity)
    tables = table_ref[...]
    slot_far = side_slots(size, edges.side, edges.other_flat)
    oper_t = operator_t(
        size, tables, gather_matrix_t(size, edges, slot_far, 0), mass_row, False
    )
    slot = side_slots(size, edges.side, edges.flat)
    rows = 2 * size.part
    first = jnp.where(edges.side >= 0, edges.side * size.part + 4 * slot, -8)
    put = jnp.concatenate([first + t for t in range(4)], axis=1)
    select = jnp.where(iota((rows, 4 * size.edges), 0) == put, 1.0, 0.0)
    points = dot_nn(select, spread_of(size, tables), None)
    part = dot_nt(points, oper_t)
    n = size.elements
    both = jnp.zeros((1, n), I32)
    hits = []
    for s in range(2):
        hit = jnp.where(edges.side == s, 1, 0)
        total = hit[:, 0:n]
        for k in range(1, 4):
            total = total + hit[:, k * n : (k + 1) * n]
        hits.append(total)
    both = jnp.where(jnp.logical_and(hits[0] > 0, hits[1] > 0), 1.0, 0.0)
    flag = jnp.max(both)
    part_ref[:, 0 : size.ops] = part
    part_ref[:, size.ops :] = jnp.full((rows, LANES - size.ops), flag, F32)


def message_kernel(size, own_ref, twin_ref, part_ref, even_ref, odd_ref):
    cells = jnp.concatenate([own_ref[0 : size.cells, :], twin_ref[0 : size.cells, :]], axis=0)
    weights = stack_left(part_ref[:, 0 : 2 * size.cells], 1)
    part = dot_nn(weights, stack_right(cells, 0), None)
    lane = iota((2 * size.part, size.wide), 1)
    part = jnp.where(lane == size.flat, part_ref[:, size.columns : size.columns + 1], part)
    part = jnp.where(lane == size.flat + 1, part_ref[:, size.ops : size.ops + 1], part)
    for s, ref in enumerate((even_ref, odd_ref)):
        first = size.cells + s * size.raw
        ref[0 : size.raw, :] = own_ref[first : first + size.raw, :]
        ref[size.raw : 2 * size.raw, :] = twin_ref[first : first + size.raw, :]
        ref[2 * size.raw :, :] = part[s * size.part : (s + 1) * size.part, :]


def inner_kernel(
    size, table_ref, own_ref, twin_ref, state_ref, sum_ref, near_ref, matrix_ref, new_ref, sem
):
    save = pltpu.make_async_copy(state_ref, new_ref, sem)
    save.start()
    parity = lax.axis_index("tile") % 2
    tables = table_ref[...]
    own, own_mass = face_edges(size, own_ref, parity)
    twin, twin_mass = face_edges(size, twin_ref, parity)
    own_slot = side_slots(size, own.side, own.other_flat)
    twin_slot = side_slots(size, twin.side, twin.other_flat)
    oper = jnp.concatenate(
        [
            operator_t(size, tables, gather_matrix_t(size, own, own_slot, 0), own_mass, False),
            operator_t(size, tables, gather_matrix_t(size, twin, twin_slot, 1), twin_mass, True),
        ],
        axis=1,
    )
    far = 2 * size.points
    targets = []
    for t in range(4):
        tt = jnp.where(own.turned == 1, 3 - t, t)
        point = 16 * own.place + edge_point(own.other_k, tt)
        local = jnp.where(own.source == 0, 0, size.points) + point
        targets.append(
            jnp.where(own.side >= 0, far + own.side * size.part + 4 * own_slot + tt, local)
        )
    target = jnp.concatenate(targets, axis=1)
    rows = far + 2 * size.part
    partner_t = jnp.where(iota((rows, 4 * size.edges), 0) == target, 1.0, 0.0)
    assemble_t = dot_nn(partner_t, spread_of(size, tables), None)
    eye = jnp.where(iota((far, size.points), 0) == iota((far, size.points), 1), 1.0, 0.0)
    total_t = dot_nn(oper, assemble_t[0:far, :] + eye)
    cells = 2 * size.cells
    matrix_ref[0 : 4 * size.raw, :] = total_t[cells : size.columns, :]
    matrix_ref[4 * size.raw : 4 * size.raw + 2 * size.part, :] = assemble_t[far:, :]
    matrix_ref[4 * size.raw + 2 * size.part :, :] = total_t[size.columns :, :]
    chip = jnp.concatenate([own_ref[0 : size.cells, :], twin_ref[0 : size.cells, :]], axis=0)
    sum_ref[...] = dot_tn(chip[:, 0 : size.flat], total_t[0:cells, :])
    side_slot = jnp.where(own.side >= 0, own.side * BLK_R + own_slot, -1)
    match = jnp.broadcast_to(twice(side_slot), (2 * size.part, 2 * size.edges)) == (
        iota((2 * size.part, 2 * size.edges), 0) // 4
    )
    t_of = iota((2 * size.part, 2 * size.edges), 0) % 4
    m_of = iota((2 * size.part, 2 * size.edges), 1) // size.edges
    weight = jnp.zeros(match.shape, F32)
    for t in range(4):
        for m in range(2):
            here = jnp.logical_and(t_of == t, m_of == m)
            weight = jnp.where(here, edge_weight(t, m), weight)
    weight = jnp.where(match, weight, 0.0)
    cell = jnp.concatenate(
        [
            4 * own.e + edge_cell(own.k, jnp.where(own.turned == 1, 1 - m, m))
            for m in range(2)
        ],
        axis=1,
    )
    cell_t = jnp.where(iota((size.cells, 2 * size.edges), 0) == cell, 1.0, 0.0)
    near_ref[...] = dot_nn(dot_nt(weight, cell_t), own_ref[0 : size.cells, :])
    save.wait()


def final_kernel(
    size,
    levels,
    even_ref,
    odd_ref,
    sum_ref,
    near_ref,
    matrix_ref,
    part_ref,
    out_ref,
    keep_ref,
    flag_ref,
):
    raw = 2 * size.raw
    mine = part_ref[0:1, size.ops : size.ops + 1]
    others = [ref[raw : raw + 1, size.flat + 1 : size.flat + 2] for ref in (even_ref, odd_ref)]
    flag = jnp.where(mine + others[0] + others[1] > 0.0, 1.0, 0.0)
    flag_ref[0, 0] = jnp.sum(flag).astype(I32)
    mass = jnp.concatenate(
        [ref[raw:, size.flat : size.flat + 1] for ref in (even_ref, odd_ref)], axis=0
    )
    part = jnp.concatenate([even_ref[raw:, :], odd_ref[raw:, :]], axis=0)
    part = part + mass * near_ref[...]
    rows = jnp.concatenate([even_ref[0:raw, :], odd_ref[0:raw, :], part], axis=0)
    n = 2 * raw + 2 * size.part
    side = matrix_ref[2 * raw : n, :]
    mass_sum = matrix_ref[n : n + 1, :] + jnp.sum(side * mass, axis=0, keepdims=True)
    keep_ref[...] = jnp.broadcast_to(mass_sum, (8, size.points))
    wide = dot_tn(stack_left(rows, 0), stack_right(matrix_ref[0:n, :], 0), None)
    total = sum_ref[...] + wide[0 : size.flat, :]
    total = total / mass_sum
    steps = levels // SUBLANES
    for f in range(size.flat // levels):
        for i in range(steps):
            row = (f * steps + i) * SUBLANES
            out_ref[pl.ds(f * levels + i, SUBLANES, stride=steps), :] = total[row : row + SUBLANES, :]


VMEM = pl.BlockSpec(memory_space=pltpu.VMEM)
SMEM = pl.BlockSpec(memory_space=pltpu.SMEM)
HBM = pl.BlockSpec(memory_space=pltpu.HBM)


def call(body, name, outs, ins, in_specs=None, out_specs=None, scratch=(), limit=8):
    return pl.pallas_call(
        body,
        out_shape=outs,
        in_specs=in_specs or [VMEM] * len(ins),
        out_specs=out_specs or [VMEM] * len(outs),
        scratch_shapes=scratch,
        compiler_params=pltpu.CompilerParams(vmem_limit_bytes=limit * 1024 * 1024),
        name=name,
    )(*ins)


def shape_of(*dims):
    return jax.ShapeDtypeStruct(dims, F32)


def advance(size, crm_state, params):
    fields, levels, lanes = crm_state.shape
    width = lanes // size.cells
    block = pltpu.VMEM((2, fields, levels, LANES), F32)
    params = [value.reshape(-1, value.shape[-1]) for value in params]
    rows = sum(value.shape[0] for value in params)
    ins = [pltpu.with_memory_space_constraint(value, pltpu.HBM) for value in (crm_state, *params)]
    return call(
        functools.partial(crm_kernel, size, levels, width, len(params)),
        "advance",
        [
            pltpu.VMEM(crm_state.shape, BF16),
            pltpu.VMEM((size.face_rows, size.wide), F32),
        ],
        ins,
        in_specs=[HBM] * len(ins),
        scratch=[pltpu.VMEM(value.shape, value.dtype) for value in params]
        + [
            pltpu.VMEM(crm_state.shape, BF16),
            pltpu.VMEM((-(-rows // SUBLANES) * SUBLANES, LANES), F32),
            block,
            block,
            pltpu.VMEM((fields, levels, LANES), F32),
            pltpu.VMEM((2 * NSUB * levels, LANES), F32),
            pltpu.VMEM((2 * NSUB * levels, 2 * LANES), F32),
            pltpu.SemaphoreType.DMA((fields,)),
            pltpu.SemaphoreType.DMA((len(params),)),
        ],
        limit=16,
    )


def swap_pairs(odd):
    tiles = lax.axis_size("tile")
    pairs = []
    for t in range(tiles):
        up = (t % 2 == 0) != odd
        pairs.append((t, (t + 1 if up else t - 1) % tiles))
    return pairs


def swap(value, odd):
    return lax.ppermute(value, "tile", swap_pairs(odd))


def shift(value, axis, steps):
    count = lax.axis_size(axis)
    return lax.ppermute(value, axis, [(s, (s + steps) % count) for s in range(count)])


def assemble_pair(size, levels, state, face):
    tables = jnp.asarray(constant_tables(size))
    twin = shift(face, "face", 1)
    (part,) = call(
        functools.partial(weights_kernel, size),
        "weights",
        [shape_of(2 * size.part, LANES)],
        [face, tables],
    )
    message = shape_of(size.tile_rows, size.wide)
    even, odd = call(
        functools.partial(message_kernel, size), "message", [message] * 2, [face, twin, part]
    )
    odd_in = swap(odd, True)
    even_in = swap(even, False)
    extra = 4 * size.raw + 2 * size.part
    inner, near, matrix, new_state = call(
        functools.partial(inner_kernel, size),
        "inner",
        [
            shape_of(size.flat, size.points),
            shape_of(2 * size.part, size.wide),
            shape_of(extra + 8, size.points),
            pltpu.HBM(state.shape, state.dtype),
        ],
        [tables, face, twin, pltpu.with_memory_space_constraint(state, pltpu.VMEM)],
        out_specs=[VMEM, VMEM, VMEM, HBM],
        scratch=[pltpu.SemaphoreType.DMA],
    )
    out, keep, flag = call(
        functools.partial(final_kernel, size, levels),
        "final",
        [
            pltpu.VMEM((size.flat, size.points), F32),
            shape_of(8, size.points),
            pltpu.SMEM((1, 1), I32),
        ],
        [even_in, odd_in, inner, near, matrix, part],
        out_specs=[VMEM, VMEM, SMEM],
    )
    return new_state, (out, part, keep, matrix, even_in, odd_in, flag)


def one_of(index, branches, *operands):
    whole = jax.make_jaxpr(lambda i, *rest: lax.switch(i, branches, *rest))(index, *operands)
    last = whole.jaxpr.eqns[-1]
    return last.primitive.bind(index, *operands, **last.params)[0]


def second_exchange(size, levels, out, part, keep, matrix, even_in, odd_in, flag):
    raw = 2 * size.raw

    def add(s, value, part, keep, matrix, even_in, odd_in):
        source = (odd_in, even_in)[s]
        first = 2 * size.cells + raw * (1 - s)
        weights = part[s * size.part : (s + 1) * size.part, first : first + raw]
        side = matrix[2 * raw + s * size.part : 2 * raw + (s + 1) * size.part, :]
        sent = jnp.dot(weights, source[0:raw, 0 : size.flat], precision=HI)
        got = swap(sent, s == 1)
        more = jnp.dot(got.T, side, precision=HI) / keep[0:1, :]
        more = more.reshape(-1, levels // SUBLANES, SUBLANES, size.points)
        return value + more.transpose(0, 2, 1, 3).reshape(value.shape)

    def none(value, *rest):
        return value

    def some(value, *rest):
        mine = rest[0][0, size.ops]
        for s, received in ((0, rest[3]), (1, rest[4])):
            other = received[raw, size.flat + 1]
            value = lax.cond(
                mine + other > 0.0, functools.partial(add, s), none, value, *rest
            )
        return value

    operands = (out, part, keep, matrix, even_in, odd_in)
    return one_of(flag[0, 0], (none, some), *operands)


def oriented(edge_lists):
    rows = []
    for code in range(8):
        side = list(edge_lists[code // 2])
        rows.append(side[::-1] if code % 2 == 1 else side)
    return np.array(rows, np.int32)


def collect(value, slots):
    pieces = [value]
    for axis, steps in (("tile", 1), ("tile", -1), ("face", 1), ("face", -1)):
        pieces.append(shift(value, axis, steps))
    return jnp.concatenate(pieces, axis=0), slots


def assemble_any(size, levels, face, masses, slots, codes):
    elements = size.elements
    cells = face[0 : size.cells, 0 : size.flat].reshape(elements, 4, size.flat)
    pool, rows = collect(cells, slots)
    pick = jnp.take(jnp.asarray(oriented(CELL_EDGE)), codes, axis=0)
    index = (rows[:, :, None] * 4 + pick).transpose(1, 0, 2).reshape(-1)
    across = jnp.take(pool.reshape(-1, size.flat), index, axis=0)
    stacked = jnp.concatenate([cells, across.reshape(elements, 8, size.flat)], axis=1)
    points = jnp.einsum("ecz,pc->epz", stacked, jnp.asarray(remap_matrix()), precision=HI)
    masses = masses.reshape(elements, 16)
    numerator, denominator = points * masses[:, :, None], masses
    weighted, rows = collect(numerator, slots)
    mass_pool, _ = collect(masses, slots)
    pick = jnp.take(jnp.asarray(oriented(GLL_EDGE)), codes, axis=0)
    for k in range(4):
        index = (rows[k][:, None] * 16 + pick[k]).reshape(-1)
        got = jnp.take(weighted.reshape(-1, size.flat), index, axis=0)
        numerator = numerator.at[:, GLL_EDGE[k]].add(got.reshape(elements, 4, size.flat))
        got = jnp.take(mass_pool.reshape(-1), index)
        denominator = denominator.at[:, GLL_EDGE[k]].add(got.reshape(elements, 4))
    ratio = (numerator / denominator[:, :, None]).reshape(size.points, size.flat)
    ratio = ratio.reshape(size.points, -1, levels // SUBLANES, SUBLANES)
    return ratio.transpose(1, 3, 2, 0).reshape(size.flat, size.points)


def local(
    crm_state,
    active_levels,
    mix_x,
    drift_speed,
    cond_rate,
    mix_z,
    point_mass,
    neighbor_slots,
    edge_codes,
):
    fields, levels, _ = crm_state.shape
    size = Sizes(neighbor_slots.shape[1], fields * levels)
    params = (
        active_levels,
        mix_x,
        drift_speed,
        cond_rate,
        mix_z,
        point_mass,
        neighbor_slots,
        edge_codes,
    )
    state, face = advance(size, crm_state, params)
    tiles = lax.axis_size("tile")
    if lax.axis_size("face") == 2 and tiles % 2 == 0 and tiles > 2:
        new_state, results = assemble_pair(size, levels, state, face)
        out = second_exchange(size, levels, *results)
    else:
        new_state = state
        out = assemble_any(size, levels, face, point_mass, neighbor_slots, edge_codes)
    return (new_state, out.reshape(fields, levels, size.points))


def solution(mesh):
    in_specs = (
        P(None, None, ("face", "tile")),
        P(("face", "tile")),
        P(("face", "tile")),
        P(("face", "tile")),
        P(("face", "tile")),
        P(),
        P(("face", "tile")),
        P(None, ("face", "tile")),
        P(None, ("face", "tile")),
    )
    out_specs = (P(None, None, ("face", "tile")), P(None, None, ("face", "tile")))
    return jax.shard_map(local, mesh=mesh, in_specs=in_specs, out_specs=out_specs, check_vma=False)
```

```python
import functools
import math

import jax
import jax.numpy as jnp
import numpy as np
from jax import lax
from jax.experimental import pallas as pl
from jax.experimental.pallas import tpu as pltpu
from jax.sharding import PartitionSpec as P

NSUB = 2
BLK_R = 4
BLK_C = 2
PER_TIME = 10.0
LANES = 128
HI = lax.Precision.HIGHEST
F32 = jnp.float32
BF16 = jnp.bfloat16
I32 = jnp.int32

CELL_EDGE = [[0, 1], [1, 3], [2, 3], [0, 2]]
GLL_EDGE = [[0, 1, 2, 3], [3, 7, 11, 15], [12, 13, 14, 15], [0, 4, 8, 12]]


def lagrange(q, z):
    centres = [-1.5, -0.5, 0.5, 1.5]
    product = 1.0
    for r in range(4):
        if r != q:
            product = product * (z - centres[r]) / (centres[q] - centres[r])
    return product


def linear_weight(j, z):
    return 0.5 - z if j == 0 else 0.5 + z


GLL_NODES = [-1.0, -1.0 / math.sqrt(5.0), 1.0 / math.sqrt(5.0), 1.0]


def remap_matrix():
    matrix = [[0.0 for column in range(12)] for row in range(16)]
    for b in range(4):
        for a in range(4):
            p = 4 * b + a
            x = GLL_NODES[a]
            y = GLL_NODES[b]
            for j in range(2):
                for i in range(2):
                    matrix[p][2 * j + i] += 0.5 * linear_weight(j, y) * lagrange(
                        1 + i, x
                    ) + 0.5 * linear_weight(i, x) * lagrange(1 + j, y)
            for m in range(2):
                matrix[p][4 + 6 + m] += 0.5 * linear_weight(m, y) * lagrange(0, x)
                matrix[p][4 + 2 + m] += 0.5 * linear_weight(m, y) * lagrange(3, x)
                matrix[p][4 + 0 + m] += 0.5 * linear_weight(m, x) * lagrange(0, y)
                matrix[p][4 + 4 + m] += 0.5 * linear_weight(m, x) * lagrange(3, y)
    return np.array(matrix, np.float32)


class Sizes:
    def __init__(self, elements, flat_len):
        self.elements = elements
        self.edges = 4 * elements
        self.cells = 4 * elements
        self.points = 16 * elements
        self.raw = 2 * BLK_R
        self.part = 4 * BLK_R
        self.flat = flat_len
        self.wide = -(-(flat_len + 2) // LANES) * LANES
        self.columns = 2 * self.cells + 4 * self.raw
        self.ops = self.columns + 8
        self.face_rows = self.cells + 2 * self.raw + 8
        self.tile_rows = 2 * self.raw + self.part


def constant_tables(size):
    matrix = remap_matrix()
    across_t = np.zeros((2 * size.edges, size.points), np.float32)
    own_t = np.zeros((size.cells, size.points), np.float32)
    spread_t = np.zeros((4 * size.edges, size.points), np.float32)
    for e in range(size.elements):
        for p in range(16):
            for c in range(4):
                own_t[4 * e + c, 16 * e + p] = matrix[p][c]
            for k in range(4):
                for m in range(2):
                    row = m * size.edges + k * size.elements + e
                    across_t[row, 16 * e + p] = matrix[p][4 + 2 * k + m]
        for k in range(4):
            for t in range(4):
                row = t * size.edges + k * size.elements + e
                spread_t[row, 16 * e + GLL_EDGE[k][t]] = 1.0
    return np.concatenate([across_t, own_t, spread_t], axis=0)


def edge_weight(t, m):
    return 0.5 * linear_weight(m, GLL_NODES[t]) * lagrange(0, -1.0)


def iota(shape, dim):
    return lax.broadcasted_iota(I32, shape, dim)


def dot_nn(a, b, precision=HI):
    return lax.dot_general(
        a, b, (((1,), (0,)), ((), ())), precision=precision, preferred_element_type=F32
    )


def dot_nt(a, b, precision=HI):
    return lax.dot_general(
        a, b, (((1,), (1,)), ((), ())), precision=precision, preferred_element_type=F32
    )


def dot_tn(a, b, precision=HI):
    return lax.dot_general(
        a, b, (((0,), (0,)), ((), ())), precision=precision, preferred_element_type=F32
    )


def split(value):
    high = value.astype(BF16)
    return high, (value - high.astype(F32)).astype(BF16)


def stack_left(value, axis):
    high, low = split(value)
    return jnp.concatenate([high, low, high], axis=axis)


def stack_right(value, axis):
    high, low = split(value)
    return jnp.concatenate([high, high, low], axis=axis)


def flat_row(table):
    return jnp.concatenate([table[k : k + 1, :] for k in range(4)], axis=1)


def twice(row):
    return jnp.concatenate([row, row], axis=1)


def side_slots(size, side, order):
    n = size.edges
    key = jnp.where(side >= 0, side * 2 * n + order, 8 * n)
    eye = iota((n, n), 0) == iota((n, n), 1)
    wide = jnp.broadcast_to(key.astype(F32), (n, n))
    column = jnp.sum(jnp.where(eye, wide, 0.0), axis=1, keepdims=True)
    floor = jnp.broadcast_to((side * 2 * n).astype(F32), (n, n))
    lower = jnp.logical_and(column < wide, column >= floor)
    count = jnp.sum(jnp.where(lower, 1.0, 0.0), axis=0, keepdims=True).astype(I32)
    return jnp.where(side >= 0, count, 0)


def edge_cell(k, m):
    odd = k & 1
    base = jnp.where(k == 2, 2, odd * jnp.where(k == 1, 1, 0))
    return base + m * (1 + odd)


def edge_point(k, t):
    odd = k & 1
    base = jnp.where(k == 2, 12, jnp.where(k == 1, 3, 0))
    return base + t * (1 + 3 * odd)


class Edges:
    def __init__(self, size, slots_row, codes_row, parity):
        n = size.edges
        flat = iota((1, n), 1)
        self.k = flat // size.elements
        self.e = flat % size.elements
        self.source = slots_row // size.elements
        self.place = slots_row % size.elements
        self.other_k = codes_row // 2
        self.turned = codes_row % 2
        self.side = jnp.where(
            self.source == 2 - parity, 0, jnp.where(self.source == 1 + parity, 1, -1)
        )
        self.flat = flat
        self.other_flat = self.other_k * size.elements + self.place


def gather_matrix_t(size, edges, slot, twin):
    cells, raw = size.cells, size.raw
    rows = []
    for m in range(2):
        mm = jnp.where(edges.turned == 1, 1 - m, m)
        cell = 4 * edges.place + edge_cell(edges.other_k, mm)
        local = jnp.where(edges.source == 0, cells * twin, cells * (1 - twin)) + cell
        far = 2 * cells + 2 * raw * edges.side + raw * twin + 2 * slot + mm
        rows.append(jnp.where(edges.side >= 0, far, local))
    target = jnp.concatenate(rows, axis=1)
    return jnp.where(iota((size.columns, 2 * size.edges), 0) == target, 1.0, 0.0)


def operator_t(size, tables, gather_t, mass_row, twin):
    across_t = tables[0 : 2 * size.edges, :]
    own_t = tables[2 * size.edges : 2 * size.edges + size.cells, :]
    from_across = dot_nn(gather_t, across_t)
    zero = jnp.zeros((size.cells, size.points), F32)
    placed = [zero, own_t] if twin else [own_t, zero]
    rest = jnp.zeros((size.columns - 2 * size.cells, size.points), F32)
    full = from_across + jnp.concatenate(placed + [rest], axis=0)
    tail = jnp.where(iota((8, size.points), 0) == 0, 1.0, 0.0)
    return jnp.concatenate([full, tail], axis=0) * mass_row


def spread_of(size, tables):
    start = 2 * size.edges + size.cells
    return tables[start : start + 4 * size.edges, :]


SUBLANES = 8


def crm_kernel(size, levels, width, count, *refs):
    state_hbm, given = refs[0], refs[1 : 1 + count]
    new_ref, face_ref = refs[1 + count : 3 + count]
    held = refs[3 + count : 3 + 2 * count]
    state_ref, table_ref, wide_ref, out_buf, base_ref, inc_ref, change_ref = refs[
        3 + 2 * count : 10 + 2 * count
    ]
    state_sem, held_sem = refs[10 + 2 * count :]
    fields = state_ref.shape[0]
    steps = levels // SUBLANES
    per_lane = LANES // width
    full = (SUBLANES, LANES)
    lane = iota(full, 1)
    pair_lanes = 2 * LANES
    pairs = size.elements // 2

    def load(f):
        return pltpu.make_async_copy(state_hbm.at[f], state_ref.at[f], state_sem.at[f])

    small = [
        pltpu.make_async_copy(src, dst, held_sem.at[n])
        for n, (src, dst) in enumerate(zip(given, held))
    ]
    for copy in small:
        copy.start()
    for f in range(fields):
        load(f).start()
    table_ref[...] = jnp.zeros(table_ref.shape, F32)
    for copy in small:
        copy.wait()
    first = 0
    for ref in held:
        rows, lanes = ref.shape
        table_ref[first : first + rows, 0:lanes] = ref[...].astype(F32)
        first += rows
    params = table_ref[...]

    def spread(ref, i):
        return ref[pl.ds(i, SUBLANES, stride=steps), :]

    eye = iota((levels, LANES), 0) == iota((levels, LANES), 1)
    mixz = jnp.broadcast_to(params[4:5, :], (levels, LANES))
    couple = jnp.sum(jnp.where(eye, mixz, 0.0), axis=1, keepdims=True)
    couple = jnp.where(iota((levels, 1), 0) < levels - 1, couple, 0.0)
    wide_ref[0, 0] = jnp.broadcast_to(couple, (levels, LANES))
    coupling = [spread(wide_ref.at[0, 0], i) for i in range(steps)]

    def vertical(a):
        above = a[1:] + [pltpu.roll(a[0], SUBLANES - 1, 0)]
        flux = [c * (u - v) for c, u, v in zip(coupling, above, a)]
        below = [pltpu.roll(flux[-1], 1, 0)] + flux[:-1]
        return [v + f - b for v, f, b in zip(a, flux, below)]

    level = [iota(full, 0) * steps + i for i in range(steps)]
    first = lane - lane % width
    east_lane = first + (lane + 1) % width
    west_lane = first + (lane + width - 1) % width

    def lanes_of(value, index):
        return jnp.take_along_axis(value, index, axis=1)

    def lanes_at(e, count=1):
        return pl.ds(pl.multiple_of(e * LANES, LANES), count * LANES)

    def column_rows(e):
        here = lanes_of(params[0:SUBLANES, :], e * per_lane + lane // width)
        active, mix, drift, rate = [
            jnp.broadcast_to(here[r : r + 1, :], full) for r in range(4)
        ]
        return active, rate, (1.0 - 2.0 * mix, mix - 0.5 * drift, mix + 0.5 * drift)

    def transport(value, weights):
        centre, east_c, west_c = weights
        east, west = lanes_of(value, east_lane), lanes_of(value, west_lane)
        return centre * value + east_c * east + west_c * west

    def transport_first(e, half):
        _, _, weights = column_rows(e)
        for f in range(fields):
            value = state_ref[f, :, lanes_at(e)].astype(F32)
            for i in range(steps):
                rows = slice(i * SUBLANES, (i + 1) * SUBLANES)
                wide_ref[half, f, rows, :] = transport(value[rows, :], weights)

    def advance_element(e, half):
        active, rate, weights = column_rows(e)
        active = active.astype(I32)
        alive = [v < active for v in level]
        ice = [jnp.where(v, 0.15, 0.0) for v in alive]

        def keep(f):
            for i in range(steps):
                out_buf[half, f, pl.ds(i, SUBLANES, stride=steps), :] = cur[f][i]
            new_ref[f, :, lanes_at(e)] = out_buf[half, f].astype(BF16)

        cur = [[spread(wide_ref.at[half, f], i) for i in range(steps)] for f in range(fields)]
        changes = []
        for substep in range(NSUB):
            if substep > 0:
                cur = [[transport(v, weights) for v in a] for a in cur]
            cur = [vertical(a) for a in cur]
            if substep == NSUB - 1:
                for f in range(4, fields):
                    keep(f)
            conds, freezes = [], []
            for i in range(steps):
                t, qv, ql, qi = [cur[f][i] for f in range(4)]
                sat = jnp.exp2((0.3 * math.log2(math.e)) * t - 1.0)
                cond = jnp.where(alive[i], jnp.maximum(rate * (qv - sat), -ql), 0.0)
                ql = ql + cond
                t = t + 0.5 * cond
                freeze = ice[i] * ql * (1.0 - jnp.tanh(t))
                cur[0][i] = t + 0.1 * freeze
                cur[1][i] = qv - cond
                cur[2][i] = ql - freeze
                cur[3][i] = qi + freeze
                conds.append(cond)
                freezes.append(freeze)
            changes += conds + freezes
        for f in range(4):
            keep(f)
        for n, value in enumerate(changes):
            change_ref[n * SUBLANES : (n + 1) * SUBLANES, half * LANES : (half + 1) * LANES] = value

    cells = pair_lanes // width
    group = iota((pair_lanes, LANES), 0) // width == iota((pair_lanes, LANES), 1) % cells
    total = jnp.where(group, 1.0, 0.0).astype(BF16)

    def set_sums(ref, p, sums):
        mine = jnp.broadcast_to(lane[0:1, :] // cells == p, sums.shape)
        ref[...] = jnp.where(mine, sums, ref[...])

    def sum_changes(p):
        change = change_ref[...]
        high = change.astype(BF16)
        low = (change - high.astype(F32)).astype(BF16)
        set_sums(inc_ref, p, dot_nn(high, total, None) + dot_nn(low, total, None))

    def pair(p, carry):
        sum_changes(p - 1)
        transport_first(2 * p + 1, 1)
        advance_element(2 * p, 0)
        for f in range(fields):
            set_sums(base_ref.at[f], p, dot_nn(state_ref[f, :, lanes_at(2 * p, 2)], total, None))
        transport_first(jnp.minimum(2 * p + 2, size.elements - 1), 0)
        advance_element(2 * p + 1, 1)
        return carry

    for f in range(fields):
        load(f).wait()
    transport_first(0, 0)
    lax.fori_loop(0, pairs, pair, 0)
    sum_changes(pairs - 1)

    def change_of(n):
        return [
            inc_ref[(n * steps + i) * SUBLANES : (n * steps + i + 1) * SUBLANES, :]
            for i in range(steps)
        ]

    parts = [[change_of(2 * n), change_of(2 * n + 1)] for n in range(NSUB)]
    parity = lax.axis_index("tile") % 2
    slots_row = flat_row(params[6:10, 0 : size.elements])
    codes_row = flat_row(params[10:14, 0 : size.elements])
    edges = Edges(size, slots_row.astype(I32), codes_row.astype(I32), parity)
    slot = side_slots(size, edges.side, edges.flat)
    rows = 2 * size.raw
    place = jnp.where(edges.side >= 0, size.cells + edges.side * size.raw + 2 * slot, -8)
    put = jnp.concatenate([place, place + 1], axis=1)
    cell = jnp.concatenate(
        [4 * edges.e + edge_cell(edges.k, m) for m in range(2)], axis=1
    )
    select = jnp.where(iota((LANES, 2 * size.edges), 0) == put, 1.0, 0.0)
    cell = jnp.broadcast_to(cell.astype(F32), (SUBLANES, 2 * size.edges))
    picked = dot_nt(cell, select, None).astype(I32)
    source = jnp.where(lane < size.cells, lane, picked)

    scale = PER_TIME / width
    columns = []
    for f in range(fields):
        start = [spread(base_ref.at[f], i) for i in range(steps)]
        mean = start
        for cond, freeze in parts:
            mean = vertical(mean)
            if f == 0:
                mean = [v + 0.5 * c + 0.1 * z for v, c, z in zip(mean, cond, freeze)]
            elif f == 1:
                mean = [v - c for v, c in zip(mean, cond)]
            elif f == 2:
                mean = [v + c - z for v, c, z in zip(mean, cond, freeze)]
            elif f == 3:
                mean = [v + z for v, z in zip(mean, freeze)]
        columns += [lanes_of(scale * (v - s), source) for v, s in zip(mean, start)]
    columns.append(jnp.zeros((size.wide - size.flat, LANES), F32))
    tendency = jnp.concatenate(columns, axis=0)
    base = size.cells + rows
    face_ref[0:base, :] = tendency.T[0:base, :]
    face_ref[base:, :] = jnp.zeros((SUBLANES, size.wide), F32)
    face_ref[base : base + 1, 0 : size.edges] = slots_row
    face_ref[base + 1 : base + 2, 0 : size.edges] = codes_row
    face_ref[base + 2 : base + 3, 0 : size.points] = params[5:6, 0 : size.points]


def face_edges(size, face_ref, parity):
    base = size.cells + 2 * size.raw
    slots_row = face_ref[base : base + 1, 0 : size.edges].astype(I32)
    codes_row = face_ref[base + 1 : base + 2, 0 : size.edges].astype(I32)
    mass_row = face_ref[base + 2 : base + 3, 0 : size.points]
    return Edges(size, slots_row, codes_row, parity), mass_row


def weights_kernel(size, own_ref, table_ref, part_ref):
    parity = lax.axis_index("tile") % 2
    edges, mass_row = face_edges(size, own_ref, parity)
    tables = table_ref[...]
    slot_far = side_slots(size, edges.side, edges.other_flat)
    oper_t = operator_t(
        size, tables, gather_matrix_t(size, edges, slot_far, 0), mass_row, False
    )
    slot = side_slots(size, edges.side, edges.flat)
    rows = 2 * size.part
    first = jnp.where(edges.side >= 0, edges.side * size.part + 4 * slot, -8)
    put = jnp.concatenate([first + t for t in range(4)], axis=1)
    select = jnp.where(iota((rows, 4 * size.edges), 0) == put, 1.0, 0.0)
    points = dot_nn(select, spread_of(size, tables), None)
    part = dot_nt(points, oper_t)
    n = size.elements
    both = jnp.zeros((1, n), I32)
    hits = []
    for s in range(2):
        hit = jnp.where(edges.side == s, 1, 0)
        total = hit[:, 0:n]
        for k in range(1, 4):
            total = total + hit[:, k * n : (k + 1) * n]
        hits.append(total)
    both = jnp.where(jnp.logical_and(hits[0] > 0, hits[1] > 0), 1.0, 0.0)
    flag = jnp.max(both)
    part_ref[:, 0 : size.ops] = part
    part_ref[:, size.ops :] = jnp.full((rows, LANES - size.ops), flag, F32)


def message_kernel(size, own_ref, twin_ref, part_ref, even_ref, odd_ref):
    cells = jnp.concatenate([own_ref[0 : size.cells, :], twin_ref[0 : size.cells, :]], axis=0)
    weights = stack_left(part_ref[:, 0 : 2 * size.cells], 1)
    part = dot_nn(weights, stack_right(cells, 0), None)
    lane = iota((2 * size.part, size.wide), 1)
    part = jnp.where(lane == size.flat, part_ref[:, size.columns : size.columns + 1], part)
    part = jnp.where(lane == size.flat + 1, part_ref[:, size.ops : size.ops + 1], part)
    for s, ref in enumerate((even_ref, odd_ref)):
        first = size.cells + s * size.raw
        ref[0 : size.raw, :] = own_ref[first : first + size.raw, :]
        ref[size.raw : 2 * size.raw, :] = twin_ref[first : first + size.raw, :]
        ref[2 * size.raw :, :] = part[s * size.part : (s + 1) * size.part, :]


def inner_kernel(
    size, table_ref, own_ref, twin_ref, state_ref, sum_ref, near_ref, matrix_ref, new_ref, sem
):
    save = pltpu.make_async_copy(state_ref, new_ref, sem)
    save.start()
    parity = lax.axis_index("tile") % 2
    tables = table_ref[...]
    own, own_mass = face_edges(size, own_ref, parity)
    twin, twin_mass = face_edges(size, twin_ref, parity)
    own_slot = side_slots(size, own.side, own.other_flat)
    twin_slot = side_slots(size, twin.side, twin.other_flat)
    oper = jnp.concatenate(
        [
            operator_t(size, tables, gather_matrix_t(size, own, own_slot, 0), own_mass, False),
            operator_t(size, tables, gather_matrix_t(size, twin, twin_slot, 1), twin_mass, True),
        ],
        axis=1,
    )
    far = 2 * size.points
    targets = []
    for t in range(4):
        tt = jnp.where(own.turned == 1, 3 - t, t)
        point = 16 * own.place + edge_point(own.other_k, tt)
        local = jnp.where(own.source == 0, 0, size.points) + point
        targets.append(
            jnp.where(own.side >= 0, far + own.side * size.part + 4 * own_slot + tt, local)
        )
    target = jnp.concatenate(targets, axis=1)
    rows = far + 2 * size.part
    partner_t = jnp.where(iota((rows, 4 * size.edges), 0) == target, 1.0, 0.0)
    assemble_t = dot_nn(partner_t, spread_of(size, tables), None)
    eye = jnp.where(iota((far, size.points), 0) == iota((far, size.points), 1), 1.0, 0.0)
    total_t = dot_nn(oper, assemble_t[0:far, :] + eye)
    cells = 2 * size.cells
    matrix_ref[0 : 4 * size.raw, :] = total_t[cells : size.columns, :]
    matrix_ref[4 * size.raw : 4 * size.raw + 2 * size.part, :] = assemble_t[far:, :]
    matrix_ref[4 * size.raw + 2 * size.part :, :] = total_t[size.columns :, :]
    chip = jnp.concatenate([own_ref[0 : size.cells, :], twin_ref[0 : size.cells, :]], axis=0)
    sum_ref[...] = dot_tn(chip[:, 0 : size.flat], total_t[0:cells, :])
    side_slot = jnp.where(own.side >= 0, own.side * BLK_R + own_slot, -1)
    match = jnp.broadcast_to(twice(side_slot), (2 * size.part, 2 * size.edges)) == (
        iota((2 * size.part, 2 * size.edges), 0) // 4
    )
    t_of = iota((2 * size.part, 2 * size.edges), 0) % 4
    m_of = iota((2 * size.part, 2 * size.edges), 1) // size.edges
    weight = jnp.zeros(match.shape, F32)
    for t in range(4):
        for m in range(2):
            here = jnp.logical_and(t_of == t, m_of == m)
            weight = jnp.where(here, edge_weight(t, m), weight)
    weight = jnp.where(match, weight, 0.0)
    cell = jnp.concatenate(
        [
            4 * own.e + edge_cell(own.k, jnp.where(own.turned == 1, 1 - m, m))
            for m in range(2)
        ],
        axis=1,
    )
    cell_t = jnp.where(iota((size.cells, 2 * size.edges), 0) == cell, 1.0, 0.0)
    near_ref[...] = dot_nn(dot_nt(weight, cell_t), own_ref[0 : size.cells, :])
    save.wait()


def final_kernel(
    size,
    levels,
    even_ref,
    odd_ref,
    sum_ref,
    near_ref,
    matrix_ref,
    part_ref,
    out_ref,
    keep_ref,
    flag_ref,
):
    raw = 2 * size.raw
    mine = part_ref[0:1, size.ops : size.ops + 1]
    others = [ref[raw : raw + 1, size.flat + 1 : size.flat + 2] for ref in (even_ref, odd_ref)]
    flag = jnp.where(mine + others[0] + others[1] > 0.0, 1.0, 0.0)
    flag_ref[0, 0] = jnp.sum(flag).astype(I32)
    mass = jnp.concatenate(
        [ref[raw:, size.flat : size.flat + 1] for ref in (even_ref, odd_ref)], axis=0
    )
    part = jnp.concatenate([even_ref[raw:, :], odd_ref[raw:, :]], axis=0)
    part = part + mass * near_ref[...]
    rows = jnp.concatenate([even_ref[0:raw, :], odd_ref[0:raw, :], part], axis=0)
    n = 2 * raw + 2 * size.part
    side = matrix_ref[2 * raw : n, :]
    mass_sum = matrix_ref[n : n + 1, :] + jnp.sum(side * mass, axis=0, keepdims=True)
    keep_ref[...] = jnp.broadcast_to(mass_sum, (8, size.points))
    wide = dot_tn(stack_left(rows, 0), stack_right(matrix_ref[0:n, :], 0), None)
    total = sum_ref[...] + wide[0 : size.flat, :]
    total = total / mass_sum
    steps = levels // SUBLANES
    for f in range(size.flat // levels):
        for i in range(steps):
            row = (f * steps + i) * SUBLANES
            out_ref[pl.ds(f * levels + i, SUBLANES, stride=steps), :] = total[row : row + SUBLANES, :]


VMEM = pl.BlockSpec(memory_space=pltpu.VMEM)
SMEM = pl.BlockSpec(memory_space=pltpu.SMEM)
HBM = pl.BlockSpec(memory_space=pltpu.HBM)


def call(body, name, outs, ins, in_specs=None, out_specs=None, scratch=(), limit=8):
    return pl.pallas_call(
        body,
        out_shape=outs,
        in_specs=in_specs or [VMEM] * len(ins),
        out_specs=out_specs or [VMEM] * len(outs),
        scratch_shapes=scratch,
        compiler_params=pltpu.CompilerParams(vmem_limit_bytes=limit * 1024 * 1024),
        name=name,
    )(*ins)


def shape_of(*dims):
    return jax.ShapeDtypeStruct(dims, F32)


def advance(size, crm_state, params):
    fields, levels, lanes = crm_state.shape
    width = lanes // size.cells
    block = pltpu.VMEM((2, fields, levels, LANES), F32)
    params = [value.reshape(-1, value.shape[-1]) for value in params]
    rows = sum(value.shape[0] for value in params)
    ins = [pltpu.with_memory_space_constraint(value, pltpu.HBM) for value in (crm_state, *params)]
    return call(
        functools.partial(crm_kernel, size, levels, width, len(params)),
        "advance",
        [
            pltpu.VMEM(crm_state.shape, BF16),
            pltpu.VMEM((size.face_rows, size.wide), F32),
        ],
        ins,
        in_specs=[HBM] * len(ins),
        scratch=[pltpu.VMEM(value.shape, value.dtype) for value in params]
        + [
            pltpu.VMEM(crm_state.shape, BF16),
            pltpu.VMEM((-(-rows // SUBLANES) * SUBLANES, LANES), F32),
            block,
            block,
            pltpu.VMEM((fields, levels, LANES), F32),
            pltpu.VMEM((2 * NSUB * levels, LANES), F32),
            pltpu.VMEM((2 * NSUB * levels, 2 * LANES), F32),
            pltpu.SemaphoreType.DMA((fields,)),
            pltpu.SemaphoreType.DMA((len(params),)),
        ],
        limit=16,
    )


def swap_pairs(odd):
    tiles = lax.axis_size("tile")
    pairs = []
    for t in range(tiles):
        up = (t % 2 == 0) != odd
        pairs.append((t, (t + 1 if up else t - 1) % tiles))
    return pairs


def swap(value, odd):
    return lax.ppermute(value, "tile", swap_pairs(odd))


def shift(value, axis, steps):
    count = lax.axis_size(axis)
    return lax.ppermute(value, axis, [(s, (s + steps) % count) for s in range(count)])


def assemble_pair(size, levels, state, face):
    tables = jnp.asarray(constant_tables(size))
    twin = shift(face, "face", 1)
    (part,) = call(
        functools.partial(weights_kernel, size),
        "weights",
        [shape_of(2 * size.part, LANES)],
        [face, tables],
    )
    message = shape_of(size.tile_rows, size.wide)
    even, odd = call(
        functools.partial(message_kernel, size), "message", [message] * 2, [face, twin, part]
    )
    odd_in = swap(odd, True)
    even_in = swap(even, False)
    extra = 4 * size.raw + 2 * size.part
    inner, near, matrix, new_state = call(
        functools.partial(inner_kernel, size),
        "inner",
        [
            shape_of(size.flat, size.points),
            shape_of(2 * size.part, size.wide),
            shape_of(extra + 8, size.points),
            pltpu.HBM(state.shape, state.dtype),
        ],
        [tables, face, twin, pltpu.with_memory_space_constraint(state, pltpu.VMEM)],
        out_specs=[VMEM, VMEM, VMEM, HBM],
        scratch=[pltpu.SemaphoreType.DMA],
    )
    out, keep, flag = call(
        functools.partial(final_kernel, size, levels),
        "final",
        [
            pltpu.VMEM((size.flat, size.points), F32),
            shape_of(8, size.points),
            pltpu.SMEM((1, 1), I32),
        ],
        [even_in, odd_in, inner, near, matrix, part],
        out_specs=[VMEM, VMEM, SMEM],
    )
    return new_state, (out, part, keep, matrix, even_in, odd_in, flag)


def one_of(index, branches, *operands):
    whole = jax.make_jaxpr(lambda i, *rest: lax.switch(i, branches, *rest))(index, *operands)
    last = whole.jaxpr.eqns[-1]
    return last.primitive.bind(index, *operands, **last.params)[0]


def second_exchange(size, levels, out, part, keep, matrix, even_in, odd_in, flag):
    raw = 2 * size.raw

    def add(s, value, part, keep, matrix, even_in, odd_in):
        source = (odd_in, even_in)[s]
        first = 2 * size.cells + raw * (1 - s)
        weights = part[s * size.part : (s + 1) * size.part, first : first + raw]
        side = matrix[2 * raw + s * size.part : 2 * raw + (s + 1) * size.part, :]
        sent = jnp.dot(weights, source[0:raw, 0 : size.flat], precision=HI)
        got = swap(sent, s == 1)
        more = jnp.dot(got.T, side, precision=HI) / keep[0:1, :]
        more = more.reshape(-1, levels // SUBLANES, SUBLANES, size.points)
        return value + more.transpose(0, 2, 1, 3).reshape(value.shape)

    def none(value, *rest):
        return value

    def some(value, *rest):
        mine = rest[0][0, size.ops]
        for s, received in ((0, rest[3]), (1, rest[4])):
            other = received[raw, size.flat + 1]
            value = lax.cond(
                mine + other > 0.0, functools.partial(add, s), none, value, *rest
            )
        return value

    operands = (out, part, keep, matrix, even_in, odd_in)
    return one_of(flag[0, 0], (none, some), *operands)


def oriented(edge_lists):
    rows = []
    for code in range(8):
        side = list(edge_lists[code // 2])
        rows.append(side[::-1] if code % 2 == 1 else side)
    return np.array(rows, np.int32)


def collect(value, slots):
    pieces = [value]
    for axis, steps in (("tile", 1), ("tile", -1), ("face", 1), ("face", -1)):
        pieces.append(shift(value, axis, steps))
    return jnp.concatenate(pieces, axis=0), slots


def assemble_any(size, levels, face, masses, slots, codes):
    elements = size.elements
    cells = face[0 : size.cells, 0 : size.flat].reshape(elements, 4, size.flat)
    pool, rows = collect(cells, slots)
    pick = jnp.take(jnp.asarray(oriented(CELL_EDGE)), codes, axis=0)
    index = (rows[:, :, None] * 4 + pick).transpose(1, 0, 2).reshape(-1)
    across = jnp.take(pool.reshape(-1, size.flat), index, axis=0)
    stacked = jnp.concatenate([cells, across.reshape(elements, 8, size.flat)], axis=1)
    points = jnp.einsum("ecz,pc->epz", stacked, jnp.asarray(remap_matrix()), precision=HI)
    masses = masses.reshape(elements, 16)
    numerator, denominator = points * masses[:, :, None], masses
    weighted, rows = collect(numerator, slots)
    mass_pool, _ = collect(masses, slots)
    pick = jnp.take(jnp.asarray(oriented(GLL_EDGE)), codes, axis=0)
    for k in range(4):
        index = (rows[k][:, None] * 16 + pick[k]).reshape(-1)
        got = jnp.take(weighted.reshape(-1, size.flat), index, axis=0)
        numerator = numerator.at[:, GLL_EDGE[k]].add(got.reshape(elements, 4, size.flat))
        got = jnp.take(mass_pool.reshape(-1), index)
        denominator = denominator.at[:, GLL_EDGE[k]].add(got.reshape(elements, 4))
    ratio = (numerator / denominator[:, :, None]).reshape(size.points, size.flat)
    ratio = ratio.reshape(size.points, -1, levels // SUBLANES, SUBLANES)
    return ratio.transpose(1, 3, 2, 0).reshape(size.flat, size.points)


def local(
    crm_state,
    active_levels,
    mix_x,
    drift_speed,
    cond_rate,
    mix_z,
    point_mass,
    neighbor_slots,
    edge_codes,
):
    fields, levels, _ = crm_state.shape
    size = Sizes(neighbor_slots.shape[1], fields * levels)
    params = (
        active_levels,
        mix_x,
        drift_speed,
        cond_rate,
        mix_z,
        point_mass,
        neighbor_slots,
        edge_codes,
    )
    state, face = advance(size, crm_state, params)
    tiles = lax.axis_size("tile")
    if lax.axis_size("face") == 2 and tiles % 2 == 0 and tiles > 2:
        new_state, results = assemble_pair(size, levels, state, face)
        out = second_exchange(size, levels, *results)
    else:
        new_state = state
        out = assemble_any(size, levels, face, point_mass, neighbor_slots, edge_codes)
    return (new_state, out.reshape(fields, levels, size.points))


def solution(mesh):
    in_specs = (
        P(None, None, ("face", "tile")),
        P(("face", "tile")),
        P(("face", "tile")),
        P(("face", "tile")),
        P(("face", "tile")),
        P(),
        P(("face", "tile")),
        P(None, ("face", "tile")),
        P(None, ("face", "tile")),
    )
    out_specs = (P(None, None, ("face", "tile")), P(None, None, ("face", "tile")))
    return jax.shard_map(local, mesh=mesh, in_specs=in_specs, out_specs=out_specs, check_vma=False)
```
